128 devices in a mesh: row: 8 (over x, core), col: 16 (over z, y).
Axes of the slice: x: 4, y: 4, z: 4, core: 2. Of those that a mesh axis runs over, the one named last changes fastest.
Arguments:
- rhs: float32 [32, 1048576], P(None, ('row', 'col')), may hold values from -12.5 to 12.5
- near_blocks: bfloat16 [16384, 4, 4096], P(('row', 'col')), may hold values from -0.1875 to 0.1875
- near_offsets: int32 [16384, 4], P(('row', 'col')), may hold values from -4 to 4, as said below
- v_factor: bfloat16 [16384, 2048], P(('row', 'col')), may hold values from -0.75 to 0.75
- mix_col: bfloat16 [8, 128, 512, 512], P('row', 'col'), may hold values from -0.25 to 0.25
- mix_row: bfloat16 [8, 256, 256, 256], P('row', 'col'), may hold values from -0.375 to 0.375
- u_factor: bfloat16 [16384, 2048], P(('row', 'col')), may hold values from -0.75 to 0.75
Outputs:
- solution: float32 [32, 1048576], P(None, ('row', 'col'))
- residual: float32 [32, 1048576], P(None, ('row', 'col'))
The draws below stay inside these ranges and needn't reach their ends.
Inputs may be any that keep to these rules, and one draw needn't show every extreme that they name: `near_offsets`: column 0 is 0; the other entries of a row are distinct and nonzero. In every aligned block of 128 rows some row holds -4 and some row holds 4.
All inputs are finite; a program needn't handle non-finite values.
Results may differ from the reference program's by a relative error of at most 0.0054.
Values may be sent and summed in bfloat16 or wider, within the bound.
A program may use at most 128 MiB of HBM per device.

```python
import jax
import jax.numpy as jnp
from jax import lax

RHS = 32
LEAF = 64
RANK = 32
NNEAR = 4
HALO = 4
LEAVES_DEV = 128
NLEAVES = 16384
N_UNKNOWNS = 1048576
SLOTS = 8
SUBSLOTS = 1
N_ROW = 8
N_COL = 16
DEVICES = 128


def draw_rhs(key, part):
    scale_key = jax.random.fold_in(key, 11)
    value_key = jax.random.fold_in(key, 12)
    scales = jnp.exp(jax.random.uniform(scale_key, (DEVICES,), jnp.float32, jnp.log(0.2), jnp.log(2.5)))
    scales = jnp.repeat(scales, N_UNKNOWNS // DEVICES)[None, :]
    values = jnp.clip(jax.random.normal(value_key, (RHS, N_UNKNOWNS), jnp.float32), -5.0, 5.0)
    return (values * scales).astype(jnp.float32)


def draw_near_offsets(key, part):
    score_key = jax.random.fold_in(key, 21)
    choices_count = 2 * HALO
    column = jnp.arange(choices_count, dtype=jnp.int32)
    candidates = jnp.where(column < HALO, column - HALO, column - HALO + 1)
    scores = jax.random.randint(score_key, (NLEAVES, choices_count), 0, 2 ** 20, dtype=jnp.int32) * choices_count + column[None, :]
    leading = (jnp.arange(NLEAVES, dtype=jnp.int32) % LEAVES_DEV == 0)[:, None]
    forced = jnp.where(column == 0, -2, jnp.where(column == choices_count - 1, -1, scores))
    scores = jnp.where(leading, forced, scores)
    order = jnp.argsort(scores, axis=1)
    picked = candidates[order[:, :NNEAR - 1]]
    return jnp.concatenate([jnp.zeros((NLEAVES, 1), jnp.int32), picked.astype(jnp.int32)], axis=1)


def shard_levels(stream_key, dims, shards, low, largest):
    loudness = 1.0
    for axis_at, shards_of in shards:
        draws = jax.random.uniform(jax.random.fold_in(jax.random.fold_in(stream_key, 6), axis_at), (shards_of,), jnp.float32, low / len(shards), largest / len(shards))
        loudness = loudness * jnp.repeat(jnp.exp(draws), dims[axis_at] // shards_of).reshape((-1,) + (1,) * (len(dims) - 1 - axis_at))
    return loudness


def normal_values(rng, shape, scale, most, split=(), held_as=jnp.bfloat16):
    level = shard_levels(rng, shape, split, -0.22, 0.18) if split else 1.0
    values = jax.random.normal(rng, shape, jnp.float32) * scale * level
    return jnp.minimum(jnp.maximum(values, -most), most).astype(held_as)


def setup_inputs(seed: int = 0) -> dict:
    arg_keys = jax.random.split(jax.random.key(seed), 8)
    rhs = draw_rhs(jax.random.fold_in(arg_keys[7], 71), 0)
    near_blocks = normal_values(arg_keys[1], (NLEAVES, NNEAR, LEAF * LEAF), (4 * NNEAR * LEAF) ** -0.5, 0.1875, ((0, 128),))
    near_offsets = draw_near_offsets(jax.random.fold_in(arg_keys[7], 71), 0)
    v_factor = normal_values(arg_keys[3], (NLEAVES, LEAF * RANK), LEAF ** -0.5, 0.75, ((0, 128),))
    mix_col = normal_values(arg_keys[4], (N_ROW, N_COL * SLOTS, N_COL * RANK, N_COL * RANK), (N_COL * RANK) ** -0.5, 0.25, ((0, 8), (1, 16)))
    mix_row = normal_values(arg_keys[5], (N_ROW * SUBSLOTS, N_COL * N_COL, N_ROW * RANK, N_ROW * RANK), (N_ROW * RANK) ** -0.5, 0.375, ((0, 8), (1, 16)))
    u_factor = normal_values(arg_keys[6], (NLEAVES, RANK * LEAF), (2 * RANK) ** -0.5, 0.75, ((0, 128),))
    return {"rhs": rhs, "near_blocks": near_blocks, "near_offsets": near_offsets, "v_factor": v_factor, "mix_col": mix_col, "mix_row": mix_row, "u_factor": u_factor}


def near_term(vector_bf, near_blocks, near_offsets):
    padded = jnp.pad(vector_bf, ((0, 0), (HALO * LEAF, HALO * LEAF)))
    padded = padded.reshape(RHS, NLEAVES + 2 * HALO, LEAF)
    blocks = near_blocks.reshape(DEVICES, LEAVES_DEV, NNEAR, LEAF, LEAF)
    offsets = near_offsets.reshape(DEVICES, LEAVES_DEV, NNEAR)

    def one_block(device):
        position = device * LEAVES_DEV + jnp.arange(LEAVES_DEV, dtype=jnp.int32)[:, None] + offsets[device] + HALO
        picked = padded[:, position, :].astype(jnp.float32)
        return jnp.einsum('slnu,lnvu->slv', picked, blocks[device].astype(jnp.float32))
    result = lax.map(one_block, jnp.arange(DEVICES, dtype=jnp.int32))
    return jnp.transpose(result, (1, 0, 2, 3)).reshape(RHS, N_UNKNOWNS)

def far_term(vector_bf, v_factor, mix_col, mix_row, u_factor):
    width_col = N_COL * RANK
    width_row = N_ROW * RANK
    local = vector_bf.reshape(RHS, NLEAVES, LEAF).astype(jnp.float32)
    factor = v_factor.reshape(NLEAVES, LEAF, RANK).astype(jnp.float32)
    coeffs = jnp.einsum('slu,luk->lsk', local, factor).astype(jnp.bfloat16)
    coeffs = coeffs.reshape(N_ROW, N_COL, N_COL, SLOTS, RHS, RANK)
    first_mix = mix_col.reshape(N_ROW, N_COL, SLOTS, N_COL, RANK, width_col)

    def level_one(rowgrp):
        return jnp.einsum('cgjsk,gjckm->gjsm', coeffs[rowgrp].astype(jnp.float32), first_mix[rowgrp].astype(jnp.float32)).astype(jnp.bfloat16)
    first = lax.map(level_one, jnp.arange(N_ROW, dtype=jnp.int32))
    first = first.reshape(N_ROW, N_COL, N_ROW, SUBSLOTS, RHS, N_COL, RANK)
    second_mix = mix_row.reshape(N_ROW, SUBSLOTS, N_COL, N_COL, N_ROW, RANK, width_row)
    expand = u_factor.reshape(N_ROW, N_COL, SUBSLOTS, N_COL, N_ROW, RANK, LEAF)

    def level_two(target):
        picked = lax.dynamic_index_in_dim(first, target, 2, keepdims=False)
        second = jnp.einsum('rgjspk,jgprkn->gjpsn', picked.astype(jnp.float32), second_mix[target].astype(jnp.float32)).astype(jnp.bfloat16)
        second = second.reshape(N_COL, SUBSLOTS, N_COL, RHS, N_ROW, RANK)
        out = jnp.einsum('gjpsqk,gjpqku->sgjpqu', second.astype(jnp.float32), expand[target].astype(jnp.float32))
        return out.reshape(RHS, N_COL * LEAVES_DEV * LEAF)
    result = lax.map(level_two, jnp.arange(N_ROW, dtype=jnp.int32))
    return jnp.transpose(result, (1, 0, 2)).reshape(RHS, N_UNKNOWNS)

def reference(rhs, near_blocks, near_offsets, v_factor, mix_col, mix_row, u_factor):

    def operator(vector):
        vector_bf = vector.astype(jnp.bfloat16)
        return vector + near_term(vector_bf, near_blocks, near_offsets) + far_term(vector_bf, v_factor, mix_col, mix_row, u_factor)
    rhs_length = jnp.sqrt(lax.optimization_barrier(jnp.sum(rhs * rhs, axis=1)))
    basis_first = rhs / rhs_length[:, None]
    image_first = operator(basis_first)
    h_one_one = lax.optimization_barrier(jnp.sum(basis_first * image_first, axis=1))
    rest_first = image_first - h_one_one[:, None] * basis_first
    h_two_one = jnp.sqrt(lax.optimization_barrier(jnp.sum(rest_first * rest_first, axis=1)))
    basis_second = rest_first / h_two_one[:, None]
    image_second = operator(basis_second)
    h_one_two = lax.optimization_barrier(jnp.sum(basis_first * image_second, axis=1))
    h_two_two = lax.optimization_barrier(jnp.sum(basis_second * image_second, axis=1))
    rest_second = image_second - h_one_two[:, None] * basis_first - h_two_two[:, None] * basis_second
    h_three_two = jnp.sqrt(lax.optimization_barrier(jnp.sum(rest_second * rest_second, axis=1)))
    m_first = h_one_one * h_one_one + h_two_one * h_two_one
    m_cross = h_one_one * h_one_two + h_two_one * h_two_two
    m_second = h_one_two * h_one_two + h_two_two * h_two_two + h_three_two * h_three_two
    determ = m_first * m_second - m_cross * m_cross
    coef_first = rhs_length * (m_second * h_one_one - m_cross * h_one_two) / determ
    coef_second = rhs_length * (m_first * h_one_two - m_cross * h_one_one) / determ
    solution = coef_first[:, None] * basis_first + coef_second[:, None] * basis_second
    residual = rhs - coef_first[:, None] * image_first - coef_second[:, None] * image_second
    return (solution, residual)
```

```python
import jax
import jax.numpy as jnp
from jax import lax
from jax.experimental import pallas as pl
from jax.experimental.pallas import tpu as pltpu
from jax.sharding import PartitionSpec as P

LEAF = 64
RANK = 32
HALO = 4
LANES = 128
QUAD = LANES // RANK
PAIRS_STEP = 16
BF16 = jnp.bfloat16
F32 = jnp.float32
MESH = pl.DeviceIdType.MESH


def iota(shape, dim):
    return lax.broadcasted_iota(jnp.int32, shape, dim)


def dot(a, b):
    return jnp.dot(a, b, preferred_element_type=F32)


def dot_t(a, b):
    return lax.dot_general(a, b, (((1,), (1,)), ((), ())), preferred_element_type=F32)


def lanes_at(index, width):
    return pl.ds(pl.multiple_of(index * width, width), width)


def regroup(tiles, group):
    out = []
    for j in range(QUAD):
        made = None
        for c in range(QUAD):
            shift = (c - j) * RANK % LANES
            moved = pltpu.roll(tiles[c], shift, 1) if shift else tiles[c]
            made = moved if made is None else jnp.where(group == c, moved, made)
        out.append(made)
    return out


def tree(parts):
    while len(parts) > 1:
        parts = [parts[i] + parts[i + 1] for i in range(0, len(parts), 2)]
    return parts[0]


def kernel(
    offs_h, rhs_h, near_h, v_h, mixc_h, mixr_h, u_h, rhs, x, y, coef,
    offs, near_raw, v_raw, mixc, mixr, u_raw,
    near_w, v_big, u_big, pick_near, pick_v, pick_u,
    xbf, xdup, nacc, left_r,
    zbuf, zrecv, tbuf, trecv, halo, part, sums,
    load_sem, halo_s, halo_r, z_s, z_r, t_s, t_r, sum_s, sum_r,
):
    n_row = lax.axis_size("row")
    n_col = lax.axis_size("col")
    total = n_row * n_col
    row = lax.axis_index("row")
    col = lax.axis_index("col")
    me = row * n_col + col
    count, width = rhs.shape
    leaves = width // LEAF
    nnear = offs.shape[0]
    slots = leaves // n_col
    tiles = slots // QUAD
    edge = HALO * LEAF

    loads = {}
    for at, (name, src, dst) in enumerate(
        (("v", v_h, v_raw), ("rhs", rhs_h, rhs), ("offs", offs_h, offs), ("near", near_h, near_raw),
         ("mixc", mixc_h, mixc), ("u", u_h, u_raw), ("mixr", mixr_h, mixr))
    ):
        loads[name] = pltpu.make_async_copy(src, dst, load_sem.at[at])
        if name in ("v", "rhs", "offs"):
            loads[name].start()

    barrier = pltpu.get_barrier_semaphore()
    before = lax.rem(me + total - 1, total)
    after = lax.rem(me + 1, total)
    before_id = (before // n_col, lax.rem(before, n_col))
    after_id = (after // n_col, lax.rem(after, n_col))
    rows = [row] + [lax.rem(row + i, n_row) for i in range(1, n_row)]
    cols = [col] + [lax.rem(col + i, n_col) for i in range(1, n_col)]
    others = [(i, j) for i in range(n_row) for j in range(n_col) if i or j]

    for i, j in others:
        pl.semaphore_signal(barrier, inc=1, device_id=(rows[i], cols[j]), device_id_type=MESH)

    lane = iota((count, LANES), 1)
    low = lane < LEAF
    group = lane // RANK

    shape = (256, 256)
    r = iota(shape, 0)
    c = iota(shape, 1)
    same = (c % 16 == r // 16) & (c // 16 % 4 == r // 4 % 4)
    pick_v[...] = jnp.where(same & (c // 64 == (r // 16 + 4 - r % 4) % 4), 1.0, 0.0).astype(BF16)
    same = (c % 16 == r // 16) & (c // 16 % 8 == r // 2 % 8)
    pick_u[...] = jnp.where(same & (c // 128 == (r // 16 + r) % 2), 1.0, 0.0).astype(BF16)
    shape = (LANES, 256)
    r = iota(shape, 0)
    c = iota(shape, 1)
    b = c % nnear
    same = (c % LANES // nnear == r % LEAF // 2) & (b // 2 == r // LEAF)
    pick_near[...] = jnp.where(same & (c // LANES == (r + b) % 2), 1.0, 0.0).astype(BF16)

    def turned(tile, shift):
        return pltpu.roll(tile, shift, 1) if shift else tile

    def prepare_v():
        lane16 = iota((16, LANES), 1) // RANK
        place = lane16 == iota((16, LANES), 0) % QUAD
        for b in range(leaves // 32):
            sides = []
            for h in range(2):
                base = b * 32 + h * 16
                raw = [v_raw[base:base + 16, t * LANES:(t + 1) * LANES].astype(F32) for t in range(16)]
                sides.append(
                    [[jnp.where(place, turned(a, d * RANK), 0.0).astype(BF16) for a in raw] for d in range(4)]
                )
            for q in range(4):
                both = jnp.concatenate(
                    [
                        jnp.concatenate([s[d][4 * q + t] for d in range(4) for t in range(4)], axis=0)
                        for s in sides
                    ],
                    axis=1,
                )
                made = dot(pick_v[...], both)
                for h in range(2):
                    for i in range(16):
                        at = (b * 32 + h * 16 + i) * LEAF + q * 16
                        v_big[at:at + 16, :] = made[i * 16:(i + 1) * 16, h * LANES:(h + 1) * LANES].astype(BF16)

    def prepare_u():
        lane16 = iota((16, LANES), 1) // LEAF
        place = lane16 == iota((16, LANES), 0) % 2
        blank = jnp.zeros((16, LANES), BF16)
        for b in range(leaves // 32):
            sides = []
            for h in range(2):
                base = b * 32 + h * 16
                raw = [u_raw[base:base + 16, t * LANES:(t + 1) * LANES].astype(F32) for t in range(16)]
                sides.append(
                    [[jnp.where(place, turned(a, d * LEAF), 0.0).astype(BF16) for a in raw] for d in range(2)]
                )
            for q in range(2):
                both = jnp.concatenate(
                    [
                        jnp.concatenate([s[d][8 * q + t] for d in range(2) for t in range(8)], axis=0)
                        for s in sides
                    ],
                    axis=1,
                )
                made = dot(pick_u[...], both)
                for h in range(2):
                    for i in range(16):
                        at = (b * 32 + h * 16 + i) * RANK + q * 16
                        side = i % QUAD // 2
                        tile = made[i * 16:(i + 1) * 16, h * LANES:(h + 1) * LANES].astype(BF16)
                        u_big[at:at + 16, side * LANES:(side + 1) * LANES] = tile
                        u_big[at:at + 16, (1 - side) * LANES:(2 - side) * LANES] = blank

    def prepare_near():
        size = nnear * LEAF // 2
        keep = (iota((size, LANES), 1) // LEAF) == iota((size, LANES), 0) % 2

        def block(b, carry):
            for k in range(PAIRS_STEP):
                pair = b * PAIRS_STEP + k
                sides = []
                for h in range(2):
                    raw = near_raw[lanes_at(pair * 2 + h, size), :].astype(F32)
                    sides.append(
                        jnp.concatenate(
                            [
                                jnp.where(keep, raw, 0.0).astype(BF16),
                                jnp.where(keep, pltpu.roll(raw, LEAF, 1), 0.0).astype(BF16),
                            ],
                            axis=0,
                        )
                    )
                made = dot(pick_near[...], jnp.concatenate(sides, axis=1))
                for h in range(2):
                    for m in range(nnear // 2):
                        near_w[lanes_at(pair * 2 + h, LEAF), m * LANES:(m + 1) * LANES] = made[
                            m * LEAF:(m + 1) * LEAF, h * LANES:(h + 1) * LANES
                        ].astype(BF16)
            return carry

        lax.fori_loop(0, leaves // 2 // PAIRS_STEP, block, 0)

    def spread(tile, first):
        swapped = pltpu.roll(tile, LEAF, 1)
        xdup[first] = jnp.where(low, tile, swapped).astype(BF16)
        xdup[first + 1] = jnp.where(low, swapped, tile).astype(BF16)

    def remote(src, dst, send, recv, to):
        return pltpu.make_async_remote_copy(
            src_ref=src, dst_ref=dst, send_sem=send, recv_sem=recv, device_id=to, device_id_type=MESH
        )

    def sum_copy(at, i, j):
        s = i * n_col + j
        return remote(part.at[at], sums.at[at, s], sum_s.at[at], sum_r.at[at], (rows[i], cols[j]))

    def sum_start(at, accs):
        spot = lane - iota((count, LANES), 0)
        spread_out = jnp.zeros((count, LANES), F32)
        for k, acc in enumerate(accs):
            spread_out = jnp.where(spot == k * count, jnp.sum(acc, axis=1, keepdims=True), spread_out)
        line = jnp.sum(spread_out, axis=0, keepdims=True)
        part[at] = line
        sums[at, 0] = line
        for i, j in others:
            sum_copy(at, i, j).start()

    def sum_finish(at, many):
        everything = remote(
            sums.at[at, 1:total], sums.at[at, 1:total], sum_s.at[at], sum_r.at[at], (rows[0], cols[1])
        )
        everything.wait_send()
        everything.wait_recv()
        line = tree([sums[at, d] for d in range(total)])
        spot = lane - iota((count, LANES), 0)
        return [jnp.sum(jnp.where(spot == k * count, line, 0.0), axis=1, keepdims=True) for k in range(many)]

    def z_dot(g4, at4):
        z = dot(xbf[:, lanes_at(at4, 256)], v_big[lanes_at(at4, 256), :])
        g, side = g4
        zbuf[g, :, side * LANES:(side + 1) * LANES] = z.astype(BF16)

    def z_copy(at, s):
        return remote(zbuf.at[cols[s]], zrecv.at[at, s], z_s.at[at, s], z_r.at[at, s], (row, cols[s]))

    def t_copy(at, s):
        return remote(tbuf.at[rows[s]], trecv.at[at, s], t_s.at[at, s], t_r.at[at, s], (rows[s], col))

    def halo_copy(at, side):
        src = xbf.at[:, width - edge:width] if side == 0 else xbf.at[:, 0:edge]
        return remote(src, halo.at[at, side], halo_s.at[at, side], halo_r.at[at, side], (after_id, before_id)[side])

    def near(b, carry):
        for k in range(PAIRS_STEP):
            pair = b * PAIRS_STEP + k
            lefts = []
            for h in range(2):
                leaf = pair * 2 + h
                picked = [xdup[leaf + HALO]] + [xdup[leaf + HALO + offs[n, leaf]] for n in range(1, nnear)]
                lefts.append(
                    jnp.concatenate(
                        [jnp.where(low, picked[2 * m], picked[2 * m + 1]) for m in range(nnear // 2)], axis=1
                    )
                )
            both = dot_t(jnp.concatenate(lefts, axis=0), near_w[lanes_at(pair, 2 * LEAF), :])
            nacc[:, lanes_at(pair, LANES)] = jnp.where(low, both[:count], both[count:])
        return carry

    steps = leaves // 2 // PAIRS_STEP

    def operator(at, out, add, dots, follow):
        for s in range(1, n_col):
            z_copy(at, s).start()
        zrecv[at, 0] = zbuf[col]
        if at == 0:
            loads["near"].wait()
            prepare_near()
            loads["offs"].wait()
        for side in range(2):
            halo_copy(at, side).wait()
        for side, beyond, first in ((0, me == 0, 0), (1, me == total - 1, leaves + HALO)):
            for k in range(HALO // 2):
                tile = halo[at, side, :, k * LANES:(k + 1) * LANES].astype(F32)
                spread(jnp.where(beyond, 0.0, tile), first + 2 * k)
        split = steps // 4 if at == 0 else steps // 2
        lax.fori_loop(0, split, near, 0)
        for s in range(1, n_col):
            z_copy(at, s).wait()
        if at == 0:
            loads["mixc"].wait()
        for jt in range(tiles):
            lefts = [[] for _ in range(QUAD)]
            for cq in range(n_col // QUAD):
                got = regroup(
                    [
                        zrecv[at, lax.rem(col + n_col - (cq * QUAD + c4), n_col), :, jt * LANES:(jt + 1) * LANES].astype(F32)
                        for c4 in range(QUAD)
                    ],
                    group,
                )
                for j4 in range(QUAD):
                    lefts[j4].append(got[j4].astype(BF16))
            for j4 in range(QUAD):
                j = jt * QUAD + j4
                tbuf[j] = dot(jnp.concatenate(lefts[j4], axis=1), mixc[j]).astype(BF16)
        for s in range(1, n_row):
            t_copy(at, s).start()
        trecv[at, 0] = tbuf[row]
        if at == 0:
            loads["u"].wait()
            prepare_u()
        lax.fori_loop(split, steps, near, 0)
        for s in range(1, n_row):
            t_copy(at, s).wait()
        if at == 0:
            loads["mixr"].wait()
        for pq in range(n_col // QUAD):
            for rq in range(n_row // QUAD):
                got = regroup(
                    [
                        trecv[at, lax.rem(row + n_row - (rq * QUAD + r4), n_row), :, pq * LANES:(pq + 1) * LANES].astype(F32)
                        for r4 in range(QUAD)
                    ],
                    group,
                )
                for p4 in range(QUAD):
                    left_r[pq * QUAD + p4, :, rq * LANES:(rq + 1) * LANES] = got[p4].astype(BF16)
        accs = [jnp.zeros((count, LANES), F32) for _ in range(len(dots) + 1)]
        for s in range(1, n_col + 1):
            p = cols[s % n_col]
            second = dot(left_r[p], mixr[p]).astype(BF16)
            for tt in range(n_row // QUAD):
                at4 = p * (n_row // QUAD) + tt
                far = dot(second[:, tt * LANES:(tt + 1) * LANES], u_big[lanes_at(at4, LANES), :])
                for k in range(2):
                    where = lanes_at(at4 * 2 + k, LANES)
                    image = nacc[:, where] + far[:, k * LANES:(k + 1) * LANES]
                    if add is not None:
                        image = add[:, where] + image
                    out[:, where] = image
                    for m, other in enumerate(dots):
                        accs[m] = accs[m] + other[:, where] * image
                    accs[-1] = accs[-1] + image * image
                    if follow:
                        xbf[:, where] = image.astype(BF16)
                        spread(image, HALO + (at4 * 2 + k) * 2)
                if follow:
                    z_dot((p, tt), at4)
        return accs

    loads["v"].wait()
    for name in ("near", "mixc", "u", "mixr"):
        loads[name].start()
    prepare_v()
    loads["rhs"].wait()
    norm = jnp.zeros((count, LANES), F32)
    for t in range(width // LANES):
        tile = rhs[:, t * LANES:(t + 1) * LANES]
        xbf[:, t * LANES:(t + 1) * LANES] = tile.astype(BF16)
        spread(tile, HALO + 2 * t)
        norm = norm + tile * tile
        if t % 2:
            g4 = t // 2
            z_dot((g4 // tiles, g4 % tiles), g4)
    pl.semaphore_wait(barrier, total - 1)
    for side in range(2):
        halo_copy(0, side).start()
    first = operator(0, x, None, (rhs,), True)
    for side in range(2):
        halo_copy(1, side).start()
    sum_start(0, [norm] + first)
    second = operator(1, y, x, (rhs, x), False)
    sum_start(1, second)
    rr, rx, xx = sum_finish(0, 3)
    ry, xy, yy = sum_finish(1, 3)

    beta = jnp.sqrt(rr)
    d = rx / rr
    h11 = 1.0 + d
    rho_sq = xx - d * rx
    rho = jnp.sqrt(rho_sq)
    h21 = rho / beta
    h12 = (ry - d * (rr + rx)) / (beta * rho)
    across = xy - d * ry
    h22 = across / rho_sq - d
    h32 = jnp.sqrt((yy - ry * ry / rr - across * across / rho_sq) / rho_sq)
    m11 = h11 * h11 + h21 * h21
    m12 = h11 * h12 + h21 * h22
    m22 = h12 * h12 + h22 * h22 + h32 * h32
    det = m11 * m22 - m12 * m12
    y1 = (m22 * h11 - m12 * h12) / det
    y2 = beta * (m11 * h12 - m12 * h11) / det
    on_x = y2 / rho
    on_r = y1 - on_x * d
    coef[0] = jnp.broadcast_to(on_r, (count, LANES))
    coef[1] = jnp.broadcast_to(on_x, (count, LANES))


CHUNKS = 4


def finish(coef, rhs, x, y, sol_h, res_h, sol, res, sem):
    count, width = rhs.shape
    on_r = coef[0]
    on_x = coef[1]
    size = width // CHUNKS
    copies = []
    for c in range(CHUNKS):
        for t in range(size // LANES):
            where = slice(c * size + t * LANES, c * size + (t + 1) * LANES)
            r_tile = rhs[:, where]
            x_tile = x[:, where]
            sol[:, where] = on_r * r_tile + on_x * x_tile
            res[:, where] = r_tile - on_r * (r_tile + x_tile) - on_x * y[:, where]
        span = slice(c * size, (c + 1) * size)
        for k, (src, dst) in enumerate(((sol, sol_h), (res, res_h))):
            copies.append(pltpu.make_async_copy(src.at[:, span], dst.at[:, span], sem.at[c, k]))
            copies[-1].start()
    for copy in copies:
        copy.wait()


def body(rhs, near_blocks, near_offsets, v_factor, mix_col, mix_row, u_factor):
    n_row = lax.axis_size("row")
    n_col = lax.axis_size("col")
    count, width = rhs.shape
    leaves, nnear = near_offsets.shape
    pieces = near_blocks.shape[2] // LANES
    near_rows = (
        near_blocks.reshape(leaves, nnear, pieces, LANES).transpose(0, 2, 1, 3).reshape(leaves * pieces * nnear, LANES)
    )
    mixc = mix_col[0]
    mixr = mix_row[0]
    slots = leaves // n_col
    total = n_row * n_col
    operands = (near_offsets.T, rhs, near_rows, v_factor, mixc, mixr, u_factor)
    vmem = pltpu.VMEM
    dma = pltpu.SemaphoreType.DMA
    field = jax.ShapeDtypeStruct((count, width), F32)
    hbm_spec = pl.BlockSpec(memory_space=pltpu.HBM)
    vmem_spec = pl.BlockSpec(memory_space=pltpu.VMEM)
    rhs_v, x, y, coef = pl.pallas_call(
        kernel,
        out_shape=(field, field, field, jax.ShapeDtypeStruct((2, count, LANES), F32)),
        in_specs=[hbm_spec] * 7,
        out_specs=(vmem_spec,) * 4,
        scratch_shapes=[
            pltpu.SMEM((nnear, leaves), jnp.int32),
            vmem(near_rows.shape, BF16),
            vmem(v_factor.shape, BF16),
            vmem(mixc.shape, BF16),
            vmem(mixr.shape, BF16),
            vmem(u_factor.shape, BF16),
            vmem((leaves * LEAF, nnear * LEAF), BF16),
            vmem((leaves * LEAF, LANES), BF16),
            vmem((leaves * RANK, 2 * LANES), BF16),
            vmem((LANES, 256), BF16),
            vmem((256, 256), BF16),
            vmem((256, 256), BF16),
            vmem((count, width), BF16),
            vmem((leaves + 2 * HALO, count, LANES), BF16),
            vmem((count, width), F32),
            vmem((n_col, count, n_row * RANK), BF16),
            vmem((n_col, count, slots * RANK), BF16),
            vmem((2, n_col, count, slots * RANK), BF16),
            vmem((n_row, count, n_col * RANK), BF16),
            vmem((2, n_row, count, n_col * RANK), BF16),
            vmem((2, 2, count, HALO * LEAF), BF16),
            vmem((2, 1, LANES), F32),
            vmem((2, total, 1, LANES), F32),
            dma((7,)),
            dma((2, 2)),
            dma((2, 2)),
            dma((2, n_col)),
            dma((2, n_col)),
            dma((2, n_row)),
            dma((2, n_row)),
            dma((2,)),
            dma((2,)),
        ],
        compiler_params=pltpu.CompilerParams(
            collective_id=0, has_side_effects=True, vmem_limit_bytes=34 * 1024 * 1024
        ),
        name="gmres",
    )(*(pltpu.with_memory_space_constraint(a, pltpu.HBM) for a in operands))
    return pl.pallas_call(
        finish,
        out_shape=(field, field),
        in_specs=[vmem_spec] * 4,
        out_specs=(hbm_spec,) * 2,
        scratch_shapes=[vmem((count, width), F32), vmem((count, width), F32), dma((CHUNKS, 2))],
        compiler_params=pltpu.CompilerParams(vmem_limit_bytes=16 * 1024 * 1024),
        name="combine",
    )(coef, rhs_v, x, y)


def solution(mesh):
    in_specs = (
        P(None, ("row", "col")),
        P(("row", "col"), None, None),
        P(("row", "col"), None),
        P(("row", "col"), None),
        P("row", "col", None, None),
        P("row", "col", None, None),
        P(("row", "col"), None),
    )
    out_specs = (P(None, ("row", "col")), P(None, ("row", "col")))
    return jax.shard_map(body, mesh=mesh, in_specs=in_specs, out_specs=out_specs, check_vma=False)
```

```python
import jax
import jax.numpy as jnp
from jax import lax
from jax.experimental import pallas as pl
from jax.experimental.pallas import tpu as pltpu
from jax.sharding import PartitionSpec as P

LEAF = 64
RANK = 32
HALO = 4
LANES = 128
QUAD = LANES // RANK
PAIRS_STEP = 16
T_GROUP = 4
Z_GROUP = 16
RING = 4
BF16 = jnp.bfloat16
F32 = jnp.float32
MESH = pl.DeviceIdType.MESH


def iota(shape, dim):
    return lax.broadcasted_iota(jnp.int32, shape, dim)


def dot(a, b):
    return jnp.dot(a, b, preferred_element_type=F32)


def dot_t(a, b):
    return lax.dot_general(a, b, (((1,), (1,)), ((), ())), preferred_element_type=F32)


def lanes_at(index, width):
    return pl.ds(pl.multiple_of(index * width, width), width)


def regroup(tiles, group):
    out = []
    for j in range(QUAD):
        made = None
        for c in range(QUAD):
            shift = (c - j) * RANK % LANES
            moved = pltpu.roll(tiles[c], shift, 1) if shift else tiles[c]
            made = moved if made is None else jnp.where(group == c, moved, made)
        out.append(made)
    return out


def tree(parts):
    while len(parts) > 1:
        parts = [parts[i] + parts[i + 1] for i in range(0, len(parts), 2)]
    return parts[0]


def kernel(
    offs_h, rhs_h, near_h, v_h, mixc_h, mixr_h, u_h, rhs, x, y, coef,
    offs, near_raw, v_raw, mixc, mixr, u_raw,
    near_w, v_big, u_big, pick_near, pick_v, pick_u,
    rim, xdup, nacc, left_c, left_r,
    zbuf, zrecv, tbuf, trecv, halo, part, early, sums,
    load_sem, halo_s, halo_r, z_s, z_r, t_s, t_r, early_s, early_r, sum_s, sum_r,
):
    n_row = lax.axis_size("row")
    n_col = lax.axis_size("col")
    total = n_row * n_col
    row = lax.axis_index("row")
    col = lax.axis_index("col")
    me = row * n_col + col
    count, width = rhs.shape
    leaves = width // LEAF
    nnear = offs.shape[0]
    slots = leaves // n_col
    tiles = slots // QUAD

    loads = {}
    for at, (name, src, dst) in enumerate(
        (("v", v_h, v_raw), ("rhs", rhs_h, rhs), ("offs", offs_h, offs), ("near", near_h, near_raw),
         ("mixc", mixc_h, mixc), ("u", u_h, u_raw), ("mixr", mixr_h, mixr))
    ):
        loads[name] = pltpu.make_async_copy(src, dst, load_sem.at[at])
        if name in ("v", "rhs", "offs"):
            loads[name].start()

    barrier = pltpu.get_barrier_semaphore()
    before = lax.rem(me + total - 1, total)
    after = lax.rem(me + 1, total)
    before_id = (before // n_col, lax.rem(before, n_col))
    after_id = (after // n_col, lax.rem(after, n_col))
    cores = n_row // RING
    place_x, place_core = row // cores, lax.rem(row, cores)
    place_z, place_y = col // RING, lax.rem(col, RING)

    def turn(base, by, size):
        return lax.rem(base + by, size) if by else base

    def away(by):
        return min(by, RING - by)

    rows = [turn(place_x, i // cores, RING) * cores + turn(place_core, i % cores, cores) for i in range(n_row)]
    cols = [turn(place_z, j // RING, RING) * RING + turn(place_y, j % RING, RING) for j in range(n_col)]

    def row_slot(r):
        dx = lax.rem(place_x + RING - r // cores, RING)
        return dx * cores + lax.rem(place_core + cores - r % cores, cores)

    def col_slot(c):
        dz = lax.rem(place_z + RING - c // RING, RING)
        return dz * RING + lax.rem(place_y + RING - c % RING, RING)

    row_far = [2 * away(i // cores) + i % cores for i in range(n_row)]
    col_far = [2 * (away(j // RING) + away(j % RING)) for j in range(n_col)]
    row_order = sorted(range(1, n_row), key=lambda i: -row_far[i])
    col_order = sorted(range(1, n_col), key=lambda j: -col_far[j])
    others = [(i, j) for i in range(n_row) for j in range(n_col) if i or j]
    others.sort(key=lambda p: -(row_far[p[0]] + col_far[p[1]]))

    greeted = [(row, cols[j]) for j in col_order] + [after_id, before_id] + [(rows[i], col) for i in row_order]
    for peer in greeted:
        pl.semaphore_signal(barrier, inc=1, device_id=peer, device_id_type=MESH)

    lane = iota((count, LANES), 1)
    low = lane < LEAF
    group = lane // RANK

    shape = (256, 256)
    r = iota(shape, 0)
    c = iota(shape, 1)
    same = (c % 16 == r // 16) & (c // 16 % 4 == r // 4 % 4)
    pick_v[...] = jnp.where(same & (c // 64 == (r // 16 + 4 - r % 4) % 4), 1.0, 0.0).astype(BF16)
    same = (c % 16 == r // 16) & (c // 16 % 8 == r // 2 % 8)
    pick_u[...] = jnp.where(same & (c // 128 == (r // 16 + r) % 2), 1.0, 0.0).astype(BF16)
    shape = (LANES, 256)
    r = iota(shape, 0)
    c = iota(shape, 1)
    b = c % nnear
    same = (c % LANES // nnear == r % LEAF // 2) & (b // 2 == r // LEAF)
    pick_near[...] = jnp.where(same & (c // LANES == (r + b) % 2), 1.0, 0.0).astype(BF16)

    def turned(tile, shift):
        return pltpu.roll(tile, shift, 1) if shift else tile

    def prepare_v():
        lane16 = iota((16, LANES), 1) // RANK
        place = lane16 == iota((16, LANES), 0) % QUAD
        for b in range(leaves // 32):
            sides = []
            for h in range(2):
                base = b * 32 + h * 16
                raw = [v_raw[base:base + 16, t * LANES:(t + 1) * LANES].astype(F32) for t in range(16)]
                sides.append(
                    [[jnp.where(place, turned(a, d * RANK), 0.0).astype(BF16) for a in raw] for d in range(4)]
                )
            for q in range(4):
                both = jnp.concatenate(
                    [
                        jnp.concatenate([s[d][4 * q + t] for d in range(4) for t in range(4)], axis=0)
                        for s in sides
                    ],
                    axis=1,
                )
                made = dot(pick_v[...], both)
                for h in range(2):
                    for i in range(16):
                        at = (b * 32 + h * 16 + i) * LEAF + q * 16
                        v_big[at:at + 16, :] = made[i * 16:(i + 1) * 16, h * LANES:(h + 1) * LANES].astype(BF16)

    def prepare_u():
        lane16 = iota((16, LANES), 1) // LEAF
        place = lane16 == iota((16, LANES), 0) % 2
        blank = jnp.zeros((16, LANES), BF16)
        for b in range(leaves // 32):
            sides = []
            for h in range(2):
                base = b * 32 + h * 16
                raw = [u_raw[base:base + 16, t * LANES:(t + 1) * LANES].astype(F32) for t in range(16)]
                sides.append(
                    [[jnp.where(place, turned(a, d * LEAF), 0.0).astype(BF16) for a in raw] for d in range(2)]
                )
            for q in range(2):
                both = jnp.concatenate(
                    [
                        jnp.concatenate([s[d][8 * q + t] for d in range(2) for t in range(8)], axis=0)
                        for s in sides
                    ],
                    axis=1,
                )
                made = dot(pick_u[...], both)
                for h in range(2):
                    for i in range(16):
                        at = (b * 32 + h * 16 + i) * RANK + q * 16
                        side = i % QUAD // 2
                        tile = made[i * 16:(i + 1) * 16, h * LANES:(h + 1) * LANES].astype(BF16)
                        u_big[at:at + 16, side * LANES:(side + 1) * LANES] = tile
                        u_big[at:at + 16, (1 - side) * LANES:(2 - side) * LANES] = blank

    def prepare_near():
        size = nnear * LEAF // 2
        keep = (iota((size, LANES), 1) // LEAF) == iota((size, LANES), 0) % 2

        def block(b, carry):
            for k in range(PAIRS_STEP):
                pair = b * PAIRS_STEP + k
                sides = []
                for h in range(2):
                    raw = near_raw[lanes_at(pair * 2 + h, size), :].astype(F32)
                    sides.append(
                        jnp.concatenate(
                            [
                                jnp.where(keep, raw, 0.0).astype(BF16),
                                jnp.where(keep, pltpu.roll(raw, LEAF, 1), 0.0).astype(BF16),
                            ],
                            axis=0,
                        )
                    )
                made = dot(pick_near[...], jnp.concatenate(sides, axis=1))
                for h in range(2):
                    for m in range(nnear // 2):
                        near_w[lanes_at(pair * 2 + h, LEAF), m * LANES:(m + 1) * LANES] = made[
                            m * LEAF:(m + 1) * LEAF, h * LANES:(h + 1) * LANES
                        ].astype(BF16)
            return carry

        lax.fori_loop(0, leaves // 2 // PAIRS_STEP, block, 0)

    def spread(tile, first):
        swapped = pltpu.roll(tile, LEAF, 1)
        xdup[first] = jnp.where(low, tile, swapped).astype(BF16)
        xdup[first + 1] = jnp.where(low, swapped, tile).astype(BF16)

    def remote(src, dst, send, recv, to):
        return pltpu.make_async_remote_copy(
            src_ref=src, dst_ref=dst, send_sem=send, recv_sem=recv, device_id=to, device_id_type=MESH
        )

    def line_of(accs):
        spot = lane - iota((count, LANES), 0)
        spread_out = jnp.zeros((count, LANES), F32)
        for k, acc in enumerate(accs):
            spread_out = jnp.where(spot == k * count, jnp.sum(acc, axis=1, keepdims=True), spread_out)
        return jnp.sum(spread_out, axis=0, keepdims=True)

    def columns_of(line, many):
        spot = lane - iota((count, LANES), 0)
        return [jnp.sum(jnp.where(spot == k * count, line, 0.0), axis=1, keepdims=True) for k in range(many)]

    def group_copy(at, s):
        to = (rows[s], col) if at == 0 else (row, cols[s])
        return remote(part.at[at], early.at[at, s], early_s.at[at, s], early_r.at[at, s], to)

    def group_start(at, line):
        part[at] = line
        early[at, 0] = line
        for s in (row_order, col_order)[at]:
            group_copy(at, s).start()

    def group_finish(at):
        for s in (row_order, col_order)[at]:
            group_copy(at, s).wait()
        return tree([early[at, d] for d in range((n_row, n_col)[at])])

    def sum_start(line):
        part[2] = line
        sums[0] = line
        for i, j in others:
            remote(part.at[2], sums.at[i * n_col + j], sum_s, sum_r, (rows[i], cols[j])).start()

    def sum_finish():
        everything = remote(sums.at[1:total], sums.at[1:total], sum_s, sum_r, (row, cols[1]))
        everything.wait_send()
        everything.wait_recv()
        return tree([sums[d] for d in range(total)])

    def z_dot(tiles_bf, at4):
        return dot(jnp.concatenate(tiles_bf, axis=1), v_big[lanes_at(at4, 256), :]).astype(BF16)

    def z_copy(at, s):
        return remote(zbuf.at[cols[s]], zrecv.at[at, s], z_s.at[at, s], z_r.at[at, s], (row, cols[s]))

    def t_copy(at, s):
        return remote(tbuf.at[rows[s]], trecv.at[at, s], t_s.at[at, s], t_r.at[at, s], (rows[s], col))

    def halo_copy(at, side):
        return remote(rim.at[at, side], halo.at[at, side], halo_s.at[at, side], halo_r.at[at, side], (after_id, before_id)[side])

    def near(b, carry):
        for k in range(PAIRS_STEP):
            pair = b * PAIRS_STEP + k
            lefts = []
            for h in range(2):
                leaf = pair * 2 + h
                picked = [xdup[leaf + HALO]] + [xdup[leaf + HALO + offs[n, leaf]] for n in range(1, nnear)]
                lefts.append(
                    jnp.concatenate(
                        [jnp.where(low, picked[2 * m], picked[2 * m + 1]) for m in range(nnear // 2)], axis=1
                    )
                )
            both = dot_t(jnp.concatenate(lefts, axis=0), near_w[lanes_at(pair, 2 * LEAF), :])
            nacc[:, lanes_at(pair, LANES)] = jnp.where(low, both[:count], both[count:])
        return carry

    steps = leaves // 2 // PAIRS_STEP

    def take(at, field, dots):
        accs = [jnp.zeros((count, LANES), F32) for _ in range(len(dots) + 1)]
        for t in range(width // LANES):
            where = slice(t * LANES, (t + 1) * LANES)
            tile = field[:, where]
            spread(tile, HALO + 2 * t)
            for m, other in enumerate(dots):
                accs[m] = accs[m] + other[:, where] * tile
            accs[-1] = accs[-1] + tile * tile
            for side, k in ((0, t - width // LANES + HALO // 2), (1, t)):
                if 0 <= k < HALO // 2:
                    rim[at, side, :, k * LANES:(k + 1) * LANES] = tile.astype(BF16)
        for side in range(2):
            halo_copy(at, side).start()
        return accs

    def operator(at, out):
        if at == 0:
            loads["near"].wait()
            prepare_near()
            loads["offs"].wait()
        lax.fori_loop(1, steps - 1, near, 0)
        for s in range(1, n_col):
            z_copy(at, s).wait()
        if at == 0:
            loads["mixc"].wait()
        for jt in range(tiles):
            for cq in range(n_col // QUAD):
                got = regroup(
                    [
                        zrecv[at, col_slot(cq * QUAD + c4), :, jt * LANES:(jt + 1) * LANES].astype(F32)
                        for c4 in range(QUAD)
                    ],
                    group,
                )
                for j4 in range(QUAD):
                    left_c[jt * QUAD + j4, :, cq * LANES:(cq + 1) * LANES] = got[j4].astype(BF16)
        for first in range(0, n_row, T_GROUP):
            ready = (row_order + [0])[first:first + T_GROUP]
            for s in ready:
                made = dot(left_c[rows[s]], mixc[rows[s]]).astype(BF16)
                if s:
                    tbuf[rows[s]] = made
                else:
                    trecv[at, 0] = made
            for s in ready:
                if s:
                    t_copy(at, s).start()
        if at == 1:
            group_start(1, group_finish(0))
        if at == 0:
            loads["u"].wait()
            prepare_u()
        for side in range(2):
            halo_copy(at, side).wait()
        for side, beyond, first in ((0, me == 0, 0), (1, me == total - 1, leaves + HALO)):
            for k in range(HALO // 2):
                tile = halo[at, side, :, k * LANES:(k + 1) * LANES].astype(F32)
                spread(jnp.where(beyond, 0.0, tile), first + 2 * k)
        for b in (0, steps - 1):
            near(b, 0)
        for s in range(1, n_row):
            t_copy(at, s).wait()
        if at == 0:
            loads["mixr"].wait()
        for pq in range(n_col // QUAD):
            for rq in range(n_row // QUAD):
                got = regroup(
                    [
                        trecv[at, row_slot(rq * QUAD + r4), :, pq * LANES:(pq + 1) * LANES].astype(F32)
                        for r4 in range(QUAD)
                    ],
                    group,
                )
                for p4 in range(QUAD):
                    left_r[pq * QUAD + p4, :, rq * LANES:(rq + 1) * LANES] = got[p4].astype(BF16)
        accs = [jnp.zeros((count, LANES), F32) for _ in range(3)]
        for first in range(0, n_col, Z_GROUP):
            ready = (col_order + [0])[first:first + Z_GROUP]
            for s in ready:
                p = cols[s]
                second = dot(left_r[p], mixr[p]).astype(BF16)
                for tt in range(tiles):
                    at4 = p * tiles + tt
                    far = dot(second[:, tt * LANES:(tt + 1) * LANES], u_big[lanes_at(at4, LANES), :])
                    made = []
                    for k in range(2):
                        where = lanes_at(at4 * 2 + k, LANES)
                        image = nacc[:, where] + far[:, k * LANES:(k + 1) * LANES]
                        if at == 1:
                            x_tile = x[:, where]
                            image = x_tile + image
                            for m, other in enumerate((rhs[:, where], x_tile, image)):
                                accs[m] = accs[m] + other * image
                        else:
                            made.append(image.astype(BF16))
                        out[:, where] = image
                    if at == 0:
                        z = z_dot(made, at4)
                        if s:
                            zbuf[p, :, tt * LANES:(tt + 1) * LANES] = z
                        else:
                            zrecv[1, 0, :, tt * LANES:(tt + 1) * LANES] = z
            if at == 0:
                for s in ready:
                    if s:
                        z_copy(1, s).start()
        return accs

    loads["v"].wait()
    for name in ("near", "mixc", "u", "mixr"):
        loads[name].start()
    prepare_v()
    loads["rhs"].wait()
    for g4 in range(leaves // QUAD):
        made = [rhs[:, t * LANES:(t + 1) * LANES].astype(BF16) for t in (2 * g4, 2 * g4 + 1)]
        zbuf[g4 // tiles, :, g4 % tiles * LANES:(g4 % tiles + 1) * LANES] = z_dot(made, g4)
    pl.semaphore_wait(barrier, len(greeted))
    for s in col_order:
        z_copy(0, s).start()
    zrecv[0, 0] = zbuf[col]
    norm = take(0, rhs, ())
    operator(0, x)
    first = take(1, x, (rhs,))
    early_line = line_of(norm + first)
    group_start(0, early_line)
    second = operator(1, y)
    sum_start(line_of(second))
    rr, rx, xx = columns_of(group_finish(1), 3)
    ry, xy, yy = columns_of(sum_finish(), 3)

    beta = jnp.sqrt(rr)
    d = rx / rr
    h11 = 1.0 + d
    rho_sq = xx - d * rx
    rho = jnp.sqrt(rho_sq)
    h21 = rho / beta
    h12 = (ry - d * (rr + rx)) / (beta * rho)
    across = xy - d * ry
    h22 = across / rho_sq - d
    h32 = jnp.sqrt((yy - ry * ry / rr - across * across / rho_sq) / rho_sq)
    m11 = h11 * h11 + h21 * h21
    m12 = h11 * h12 + h21 * h22
    m22 = h12 * h12 + h22 * h22 + h32 * h32
    det = m11 * m22 - m12 * m12
    y1 = (m22 * h11 - m12 * h12) / det
    y2 = beta * (m11 * h12 - m12 * h11) / det
    on_x = y2 / rho
    on_r = y1 - on_x * d
    coef[0] = jnp.broadcast_to(on_r, (count, LANES))
    coef[1] = jnp.broadcast_to(on_x, (count, LANES))


CHUNKS = 4


def finish(coef, rhs, x, y, sol_h, res_h, sol, res, sem):
    count, width = rhs.shape
    on_r = coef[0]
    on_x = coef[1]
    size = width // CHUNKS
    copies = []
    for c in range(CHUNKS):
        for t in range(size // LANES):
            where = slice(c * size + t * LANES, c * size + (t + 1) * LANES)
            r_tile = rhs[:, where]
            x_tile = x[:, where]
            sol[:, where] = on_r * r_tile + on_x * x_tile
            res[:, where] = r_tile - on_r * (r_tile + x_tile) - on_x * y[:, where]
        span = slice(c * size, (c + 1) * size)
        for k, (src, dst) in enumerate(((sol, sol_h), (res, res_h))):
            copies.append(pltpu.make_async_copy(src.at[:, span], dst.at[:, span], sem.at[c, k]))
            copies[-1].start()
    for copy in copies:
        copy.wait()


def body(rhs, near_blocks, near_offsets, v_factor, mix_col, mix_row, u_factor):
    n_row = lax.axis_size("row")
    n_col = lax.axis_size("col")
    count, width = rhs.shape
    leaves, nnear = near_offsets.shape
    pieces = near_blocks.shape[2] // LANES
    near_rows = (
        near_blocks.reshape(leaves, nnear, pieces, LANES).transpose(0, 2, 1, 3).reshape(leaves * pieces * nnear, LANES)
    )
    mixc = mix_col[0]
    mixr = mix_row[0]
    slots = leaves // n_col
    total = n_row * n_col
    operands = (near_offsets.T, rhs, near_rows, v_factor, mixc, mixr, u_factor)
    vmem = pltpu.VMEM
    dma = pltpu.SemaphoreType.DMA
    field = jax.ShapeDtypeStruct((count, width), F32)
    hbm_spec = pl.BlockSpec(memory_space=pltpu.HBM)
    vmem_spec = pl.BlockSpec(memory_space=pltpu.VMEM)
    rhs_v, x, y, coef = pl.pallas_call(
        kernel,
        out_shape=(field, field, field, jax.ShapeDtypeStruct((2, count, LANES), F32)),
        in_specs=[hbm_spec] * 7,
        out_specs=(vmem_spec,) * 4,
        scratch_shapes=[
            pltpu.SMEM((nnear, leaves), jnp.int32),
            vmem(near_rows.shape, BF16),
            vmem(v_factor.shape, BF16),
            vmem(mixc.shape, BF16),
            vmem(mixr.shape, BF16),
            vmem(u_factor.shape, BF16),
            vmem((leaves * LEAF, nnear * LEAF), BF16),
            vmem((leaves * LEAF, LANES), BF16),
            vmem((leaves * RANK, 2 * LANES), BF16),
            vmem((LANES, 256), BF16),
            vmem((256, 256), BF16),
            vmem((256, 256), BF16),
            vmem((2, 2, count, HALO * LEAF), BF16),
            vmem((leaves + 2 * HALO, count, LANES), BF16),
            vmem((count, width), F32),
            vmem((slots, count, n_col * RANK), BF16),
            vmem((n_col, count, n_row * RANK), BF16),
            vmem((n_col, count, slots * RANK), BF16),
            vmem((2, n_col, count, slots * RANK), BF16),
            vmem((n_row, count, n_col * RANK), BF16),
            vmem((2, n_row, count, n_col * RANK), BF16),
            vmem((2, 2, count, HALO * LEAF), BF16),
            vmem((3, 1, LANES), F32),
            vmem((2, n_col, 1, LANES), F32),
            vmem((total, 1, LANES), F32),
            dma((7,)),
            dma((2, 2)),
            dma((2, 2)),
            dma((2, n_col)),
            dma((2, n_col)),
            dma((2, n_row)),
            dma((2, n_row)),
            dma((2, n_col)),
            dma((2, n_col)),
            dma(()),
            dma(()),
        ],
        compiler_params=pltpu.CompilerParams(
            collective_id=0, has_side_effects=True, vmem_limit_bytes=34 * 1024 * 1024
        ),
        name="gmres",
    )(*(pltpu.with_memory_space_constraint(a, pltpu.HBM) for a in operands))
    return pl.pallas_call(
        finish,
        out_shape=(field, field),
        in_specs=[vmem_spec] * 4,
        out_specs=(hbm_spec,) * 2,
        scratch_shapes=[vmem((count, width), F32), vmem((count, width), F32), dma((CHUNKS, 2))],
        compiler_params=pltpu.CompilerParams(vmem_limit_bytes=16 * 1024 * 1024),
        name="combine",
    )(coef, rhs_v, x, y)


def solution(mesh):
    in_specs = (
        P(None, ("row", "col")),
        P(("row", "col"), None, None),
        P(("row", "col"), None),
        P(("row", "col"), None),
        P("row", "col", None, None),
        P("row", "col", None, None),
        P(("row", "col"), None),
    )
    out_specs = (P(None, ("row", "col")), P(None, ("row", "col")))
    return jax.shard_map(body, mesh=mesh, in_specs=in_specs, out_specs=out_specs, check_vma=False)
```

```python
import jax
import jax.numpy as jnp
from jax import lax
from jax.experimental import pallas as pl
from jax.experimental.pallas import tpu as pltpu
from jax.sharding import PartitionSpec as P

LEAF = 64
RANK = 32
HALO = 4
LANES = 128
QUAD = LANES // RANK
PAIRS_STEP = 16
RING = 4
BF16 = jnp.bfloat16
F32 = jnp.float32
MESH = pl.DeviceIdType.MESH


def iota(shape, dim):
    return lax.broadcasted_iota(jnp.int32, shape, dim)


def dot(a, b):
    return jnp.dot(a, b, preferred_element_type=F32)


def dot_t(a, b):
    return lax.dot_general(a, b, (((1,), (1,)), ((), ())), preferred_element_type=F32)


def lanes_at(index, width):
    return pl.ds(pl.multiple_of(index * width, width), width)


def regroup(tiles, group):
    out = []
    for j in range(QUAD):
        made = None
        for c in range(QUAD):
            shift = (c - j) * RANK % LANES
            moved = pltpu.roll(tiles[c], shift, 1) if shift else tiles[c]
            made = moved if made is None else jnp.where(group == c, moved, made)
        out.append(made)
    return out


def tree(parts):
    while len(parts) > 1:
        parts = [parts[i] + parts[i + 1] for i in range(0, len(parts), 2)]
    return parts[0]


def kernel(
    offs_h, rhs_h, near_h, v_h, mixc_h, mixr_h, u_h, rhs, x, y, coef,
    offs, near_raw, v_raw, mixc, mixr, u_raw,
    near_w, v_big, u_big, pick_near, pick_v, pick_u,
    rim, xdup, nacc, left_c, left_r, right,
    zbuf, zrecv, tbuf, trecv, halo, part, early, sums,
    load_sem, halo_s, halo_r, z_s, z_r, t_s, t_r, early_s, early_r, sum_s, sum_r,
):
    n_row = lax.axis_size("row")
    n_col = lax.axis_size("col")
    total = n_row * n_col
    row = lax.axis_index("row")
    col = lax.axis_index("col")
    me = row * n_col + col
    count, width = rhs.shape
    leaves = width // LEAF
    nnear = offs.shape[0]
    slots = leaves // n_col
    tiles = slots // QUAD

    loads = {}
    for at, (name, src, dst) in enumerate(
        (("v", v_h, v_raw), ("rhs", rhs_h, rhs), ("offs", offs_h, offs), ("near", near_h, near_raw),
         ("mixc", mixc_h, mixc), ("u", u_h, u_raw), ("mixr", mixr_h, mixr))
    ):
        loads[name] = pltpu.make_async_copy(src, dst, load_sem.at[at])
        if name in ("v", "rhs", "offs"):
            loads[name].start()

    barrier = pltpu.get_barrier_semaphore()
    before = lax.rem(me + total - 1, total)
    after = lax.rem(me + 1, total)
    before_id = (before // n_col, lax.rem(before, n_col))
    after_id = (after // n_col, lax.rem(after, n_col))
    cores = n_row // RING
    place_x, place_core = row // cores, lax.rem(row, cores)
    place_z, place_y = col // RING, lax.rem(col, RING)

    def turn(base, by, size):
        return lax.rem(base + by, size) if by else base

    def away(by):
        return min(by, RING - by)

    rows = [turn(place_x, i // cores, RING) * cores + turn(place_core, i % cores, cores) for i in range(n_row)]
    cols = [turn(place_z, j // RING, RING) * RING + turn(place_y, j % RING, RING) for j in range(n_col)]

    def row_slot(r):
        dx = lax.rem(place_x + RING - r // cores, RING)
        return dx * cores + lax.rem(place_core + cores - r % cores, cores)

    def col_slot(c):
        dz = lax.rem(place_z + RING - c // RING, RING)
        return dz * RING + lax.rem(place_y + RING - c % RING, RING)

    row_far = [2 * away(i // cores) + i % cores for i in range(n_row)]
    col_far = [2 * (away(j // RING) + away(j % RING)) for j in range(n_col)]
    odd = lax.rem(place_x, 2)
    halves = (1 - place_x // 2, place_x // 2)
    targets = (
        ((2, 0), (2, 1), (3 - 2 * odd, 0), (3 - 2 * odd, 1)),
        ((1 + 2 * odd, 0), (1 + 2 * odd, 1), (0, 1), (None, 0)),
    )
    row_order = sorted(range(1, n_row), key=lambda i: -row_far[i])
    col_order = sorted(range(1, n_col), key=lambda j: -col_far[j])
    others = [(i, j) for i in range(n_row) for j in range(n_col) if i or j]
    others.sort(key=lambda p: -(row_far[p[0]] + col_far[p[1]]))

    greeted = [(row, cols[j]) for j in col_order] + [after_id, before_id] + [(rows[i], col) for i in row_order]
    for peer in greeted:
        pl.semaphore_signal(barrier, inc=1, device_id=peer, device_id_type=MESH)

    lane = iota((count, LANES), 1)
    low = lane < LEAF
    group = lane // RANK

    shape = (256, 256)
    r = iota(shape, 0)
    c = iota(shape, 1)
    same = (c % 16 == r // 16) & (c // 16 % 4 == r // 4 % 4)
    pick_v[...] = jnp.where(same & (c // 64 == (r // 16 + 4 - r % 4) % 4), 1.0, 0.0).astype(BF16)
    same = (c % 16 == r // 16) & (c // 16 % 8 == r // 2 % 8)
    pick_u[...] = jnp.where(same & (c // 128 == (r // 16 + r) % 2), 1.0, 0.0).astype(BF16)
    shape = (LANES, 256)
    r = iota(shape, 0)
    c = iota(shape, 1)
    b = c % nnear
    same = (c % LANES // nnear == r % LEAF // 2) & (b // 2 == r // LEAF)
    pick_near[...] = jnp.where(same & (c // LANES == (r + b) % 2), 1.0, 0.0).astype(BF16)

    def turned(tile, shift):
        return pltpu.roll(tile, shift, 1) if shift else tile

    def prepare_v():
        lane16 = iota((16, LANES), 1) // RANK
        place = lane16 == iota((16, LANES), 0) % QUAD
        for b in range(leaves // 32):
            sides = []
            for h in range(2):
                base = b * 32 + h * 16
                raw = [v_raw[base:base + 16, t * LANES:(t + 1) * LANES].astype(F32) for t in range(16)]
                sides.append(
                    [[jnp.where(place, turned(a, d * RANK), 0.0).astype(BF16) for a in raw] for d in range(4)]
                )
            for q in range(4):
                both = jnp.concatenate(
                    [
                        jnp.concatenate([s[d][4 * q + t] for d in range(4) for t in range(4)], axis=0)
                        for s in sides
                    ],
                    axis=1,
                )
                made = dot(pick_v[...], both)
                for h in range(2):
                    for i in range(16):
                        at = (b * 32 + h * 16 + i) * LEAF + q * 16
                        v_big[at:at + 16, :] = made[i * 16:(i + 1) * 16, h * LANES:(h + 1) * LANES].astype(BF16)

    def prepare_u():
        lane16 = iota((16, LANES), 1) // LEAF
        place = lane16 == iota((16, LANES), 0) % 2
        blank = jnp.zeros((16, LANES), BF16)
        for b in range(leaves // 32):
            sides = []
            for h in range(2):
                base = b * 32 + h * 16
                raw = [u_raw[base:base + 16, t * LANES:(t + 1) * LANES].astype(F32) for t in range(16)]
                sides.append(
                    [[jnp.where(place, turned(a, d * LEAF), 0.0).astype(BF16) for a in raw] for d in range(2)]
                )
            for q in range(2):
                both = jnp.concatenate(
                    [
                        jnp.concatenate([s[d][8 * q + t] for d in range(2) for t in range(8)], axis=0)
                        for s in sides
                    ],
                    axis=1,
                )
                made = dot(pick_u[...], both)
                for h in range(2):
                    for i in range(16):
                        at = (b * 32 + h * 16 + i) * RANK + q * 16
                        side = i % QUAD // 2
                        tile = made[i * 16:(i + 1) * 16, h * LANES:(h + 1) * LANES].astype(BF16)
                        u_big[at:at + 16, side * LANES:(side + 1) * LANES] = tile
                        u_big[at:at + 16, (1 - side) * LANES:(2 - side) * LANES] = blank

    def prepare_near():
        size = nnear * LEAF // 2
        keep = (iota((size, LANES), 1) // LEAF) == iota((size, LANES), 0) % 2

        def block(b, carry):
            for k in range(PAIRS_STEP):
                pair = b * PAIRS_STEP + k
                sides = []
                for h in range(2):
                    raw = near_raw[lanes_at(pair * 2 + h, size), :].astype(F32)
                    sides.append(
                        jnp.concatenate(
                            [
                                jnp.where(keep, raw, 0.0).astype(BF16),
                                jnp.where(keep, pltpu.roll(raw, LEAF, 1), 0.0).astype(BF16),
                            ],
                            axis=0,
                        )
                    )
                made = dot(pick_near[...], jnp.concatenate(sides, axis=1))
                for h in range(2):
                    for m in range(nnear // 2):
                        near_w[lanes_at(pair * 2 + h, LEAF), m * LANES:(m + 1) * LANES] = made[
                            m * LEAF:(m + 1) * LEAF, h * LANES:(h + 1) * LANES
                        ].astype(BF16)
            return carry

        lax.fori_loop(0, leaves // 2 // PAIRS_STEP, block, 0)

    def spread(tile, first):
        swapped = pltpu.roll(tile, LEAF, 1)
        xdup[first] = jnp.where(low, tile, swapped).astype(BF16)
        xdup[first + 1] = jnp.where(low, swapped, tile).astype(BF16)

    def remote(src, dst, send, recv, to):
        return pltpu.make_async_remote_copy(
            src_ref=src, dst_ref=dst, send_sem=send, recv_sem=recv, device_id=to, device_id_type=MESH
        )

    def line_of(accs):
        spot = lane - iota((count, LANES), 0)
        spread_out = jnp.zeros((count, LANES), F32)
        for k, acc in enumerate(accs):
            spread_out = jnp.where(spot == k * count, jnp.sum(acc, axis=1, keepdims=True), spread_out)
        return jnp.sum(spread_out, axis=0, keepdims=True)

    def columns_of(line, many):
        spot = lane - iota((count, LANES), 0)
        return [jnp.sum(jnp.where(spot == k * count, line, 0.0), axis=1, keepdims=True) for k in range(many)]

    def group_copy(at, s):
        to = (rows[s], col) if at == 0 else (row, cols[s])
        return remote(part.at[at], early.at[at, s], early_s.at[at, s], early_r.at[at, s], to)

    def group_start(at, line):
        part[at] = line
        early[at, 0] = line
        for s in (row_order, col_order)[at]:
            group_copy(at, s).start()

    def group_finish(at):
        for s in (row_order, col_order)[at]:
            group_copy(at, s).wait()
        return tree([early[at, d] for d in range((n_row, n_col)[at])])

    def sum_start(line):
        part[2] = line
        sums[0] = line
        for i, j in others:
            remote(part.at[2], sums.at[i * n_col + j], sum_s, sum_r, (rows[i], cols[j])).start()

    def sum_finish():
        everything = remote(sums.at[1:total], sums.at[1:total], sum_s, sum_r, (row, cols[1]))
        everything.wait_send()
        everything.wait_recv()
        return tree([sums[d] for d in range(total)])

    def z_pass(at, h, field):
        for s in col_order + [0]:
            at4 = cols[s] * tiles + halves[h]
            made = jnp.concatenate(
                [field[:, lanes_at(at4 * 2 + k, LANES)].astype(BF16) for k in range(2)], axis=1
            )
            z = dot(made, v_big[lanes_at(at4, 256), :]).astype(BF16)
            if s:
                zbuf[h, cols[s]] = z
            else:
                zrecv[at, h, 0] = z

    def z_copy(at, h, s):
        return remote(
            zbuf.at[h, cols[s]], zrecv.at[at, h, s], z_s.at[at, h, s], z_r.at[at, h, s], (row, cols[s])
        )

    def t_copy(at, s, to):
        return remote(tbuf.at[to], trecv.at[at, s], t_s.at[at, s], t_r.at[at, s], (to, col))

    def halo_copy(at, side):
        return remote(rim.at[at, side], halo.at[at, side], halo_s.at[at, side], halo_r.at[at, side], (after_id, before_id)[side])

    def near(b, carry):
        for k in range(PAIRS_STEP):
            pair = b * PAIRS_STEP + k
            lefts = []
            for h in range(2):
                leaf = pair * 2 + h
                picked = [xdup[leaf + HALO]] + [xdup[leaf + HALO + offs[n, leaf]] for n in range(1, nnear)]
                lefts.append(
                    jnp.concatenate(
                        [jnp.where(low, picked[2 * m], picked[2 * m + 1]) for m in range(nnear // 2)], axis=1
                    )
                )
            both = dot_t(jnp.concatenate(lefts, axis=0), near_w[lanes_at(pair, 2 * LEAF), :])
            nacc[:, lanes_at(pair, LANES)] = jnp.where(low, both[:count], both[count:])
        return carry

    steps = leaves // 2 // PAIRS_STEP

    def take(at, field, dots):
        accs = [jnp.zeros((count, LANES), F32) for _ in range(len(dots) + 1)]
        for t in range(width // LANES):
            where = slice(t * LANES, (t + 1) * LANES)
            tile = field[:, where]
            spread(tile, HALO + 2 * t)
            for m, other in enumerate(dots):
                accs[m] = accs[m] + other[:, where] * tile
            accs[-1] = accs[-1] + tile * tile
            for side, k in ((0, t - width // LANES + HALO // 2), (1, t)):
                if 0 <= k < HALO // 2:
                    rim[at, side, :, k * LANES:(k + 1) * LANES] = tile.astype(BF16)
        for side in range(2):
            halo_copy(at, side).start()
        return accs

    def operator(at, out):
        if at == 0:
            loads["near"].wait()
            prepare_near()
            loads["offs"].wait()
        lax.fori_loop(1, steps - 1, near, 0)
        for h in range(2):
            for s in range(1, n_col):
                z_copy(at, h, s).wait()
            if at == 0 and h == 0:
                loads["mixc"].wait()
            for cq in range(n_col // QUAD):
                got = regroup([zrecv[at, h, col_slot(cq * QUAD + c4)].astype(F32) for c4 in range(QUAD)], group)
                for j4 in range(QUAD):
                    left_c[h, j4, :, cq * LANES:(cq + 1) * LANES] = got[j4].astype(BF16)
            ready = []
            for dx, dc in targets[h]:
                to = lax.rem(place_x + (0 if dx is None else dx), RING) * cores + turn(place_core, dc, cores)
                made = dot(left_c[h, lax.rem(to, QUAD)], mixc[to]).astype(BF16)
                if dx is None:
                    trecv[at, 0] = made
                else:
                    tbuf[to] = made
                    ready.append((dx * cores + dc, to))
            for s, to in ready:
                t_copy(at, s, to).start()
        if at == 1:
            group_start(1, group_finish(0))
        if at == 0:
            loads["u"].wait()
            prepare_u()
        for side in range(2):
            halo_copy(at, side).wait()
        for side, beyond, first in ((0, me == 0, 0), (1, me == total - 1, leaves + HALO)):
            for k in range(HALO // 2):
                tile = halo[at, side, :, k * LANES:(k + 1) * LANES].astype(F32)
                spread(jnp.where(beyond, 0.0, tile), first + 2 * k)
        for b in (0, steps - 1):
            near(b, 0)
        for s in range(1, n_row):
            t_copy(at, s, rows[s]).wait()
        if at == 0:
            loads["mixr"].wait()
        for pq in range(n_col // QUAD):
            for rq in range(n_row // QUAD):
                got = regroup(
                    [
                        trecv[at, row_slot(rq * QUAD + r4), :, pq * LANES:(pq + 1) * LANES].astype(F32)
                        for r4 in range(QUAD)
                    ],
                    group,
                )
                for p4 in range(QUAD):
                    left_r[pq * QUAD + p4, :, rq * LANES:(rq + 1) * LANES] = got[p4].astype(BF16)
        for p in range(n_col):
            right[p] = dot(left_r[p], mixr[p]).astype(BF16)
        accs = [jnp.zeros((count, LANES), F32) for _ in range(3)]
        for p in range(n_col):
            for tt in range(tiles):
                at4 = p * tiles + tt
                far = dot(right[p, :, tt * LANES:(tt + 1) * LANES], u_big[at4 * LANES:(at4 + 1) * LANES, :])
                for k in range(2):
                    where = slice((at4 * 2 + k) * LANES, (at4 * 2 + k + 1) * LANES)
                    image = nacc[:, where] + far[:, k * LANES:(k + 1) * LANES]
                    if at == 1:
                        x_tile = x[:, where]
                        image = x_tile + image
                        for m, other in enumerate((rhs[:, where], x_tile, image)):
                            accs[m] = accs[m] + other * image
                    out[:, where] = image
        return accs

    loads["v"].wait()
    for name in ("near", "mixc", "u", "mixr"):
        loads[name].start()
    prepare_v()
    loads["rhs"].wait()
    for h in range(2):
        z_pass(0, h, rhs)
    pl.semaphore_wait(barrier, len(greeted))
    for h in range(2):
        for s in col_order:
            z_copy(0, h, s).start()
    norm = take(0, rhs, ())
    operator(0, x)
    for h in range(2):
        z_pass(1, h, x)
        for s in col_order:
            z_copy(1, h, s).start()
    first = take(1, x, (rhs,))
    early_line = line_of(norm + first)
    group_start(0, early_line)
    second = operator(1, y)
    sum_start(line_of(second))
    rr, rx, xx = columns_of(group_finish(1), 3)
    ry, xy, yy = columns_of(sum_finish(), 3)

    beta = jnp.sqrt(rr)
    d = rx / rr
    h11 = 1.0 + d
    rho_sq = xx - d * rx
    rho = jnp.sqrt(rho_sq)
    h21 = rho / beta
    h12 = (ry - d * (rr + rx)) / (beta * rho)
    across = xy - d * ry
    h22 = across / rho_sq - d
    h32 = jnp.sqrt((yy - ry * ry / rr - across * across / rho_sq) / rho_sq)
    m11 = h11 * h11 + h21 * h21
    m12 = h11 * h12 + h21 * h22
    m22 = h12 * h12 + h22 * h22 + h32 * h32
    det = m11 * m22 - m12 * m12
    y1 = (m22 * h11 - m12 * h12) / det
    y2 = beta * (m11 * h12 - m12 * h11) / det
    on_x = y2 / rho
    on_r = y1 - on_x * d
    coef[0] = jnp.broadcast_to(on_r, (count, LANES))
    coef[1] = jnp.broadcast_to(on_x, (count, LANES))


CHUNKS = 4


def finish(coef, rhs, x, y, sol_h, res_h, sol, res, sem):
    count, width = rhs.shape
    on_r = coef[0]
    on_x = coef[1]
    size = width // CHUNKS
    copies = []
    for c in range(CHUNKS):
        for t in range(size // LANES):
            where = slice(c * size + t * LANES, c * size + (t + 1) * LANES)
            r_tile = rhs[:, where]
            x_tile = x[:, where]
            sol[:, where] = on_r * r_tile + on_x * x_tile
            res[:, where] = r_tile - on_r * (r_tile + x_tile) - on_x * y[:, where]
        span = slice(c * size, (c + 1) * size)
        for k, (src, dst) in enumerate(((sol, sol_h), (res, res_h))):
            copies.append(pltpu.make_async_copy(src.at[:, span], dst.at[:, span], sem.at[c, k]))
            copies[-1].start()
    for copy in copies:
        copy.wait()


def body(rhs, near_blocks, near_offsets, v_factor, mix_col, mix_row, u_factor):
    n_row = lax.axis_size("row")
    n_col = lax.axis_size("col")
    count, width = rhs.shape
    leaves, nnear = near_offsets.shape
    pieces = near_blocks.shape[2] // LANES
    near_rows = (
        near_blocks.reshape(leaves, nnear, pieces, LANES).transpose(0, 2, 1, 3).reshape(leaves * pieces * nnear, LANES)
    )
    mixc = mix_col[0]
    mixr = mix_row[0]
    slots = leaves // n_col
    total = n_row * n_col
    operands = (near_offsets.T, rhs, near_rows, v_factor, mixc, mixr, u_factor)
    vmem = pltpu.VMEM
    dma = pltpu.SemaphoreType.DMA
    field = jax.ShapeDtypeStruct((count, width), F32)
    hbm_spec = pl.BlockSpec(memory_space=pltpu.HBM)
    vmem_spec = pl.BlockSpec(memory_space=pltpu.VMEM)
    rhs_v, x, y, coef = pl.pallas_call(
        kernel,
        out_shape=(field, field, field, jax.ShapeDtypeStruct((2, count, LANES), F32)),
        in_specs=[hbm_spec] * 7,
        out_specs=(vmem_spec,) * 4,
        scratch_shapes=[
            pltpu.SMEM((nnear, leaves), jnp.int32),
            vmem(near_rows.shape, BF16),
            vmem(v_factor.shape, BF16),
            vmem(mixc.shape, BF16),
            vmem(mixr.shape, BF16),
            vmem(u_factor.shape, BF16),
            vmem((leaves * LEAF, nnear * LEAF), BF16),
            vmem((leaves * LEAF, LANES), BF16),
            vmem((leaves * RANK, 2 * LANES), BF16),
            vmem((LANES, 256), BF16),
            vmem((256, 256), BF16),
            vmem((256, 256), BF16),
            vmem((2, 2, count, HALO * LEAF), BF16),
            vmem((leaves + 2 * HALO, count, LANES), BF16),
            vmem((count, width), F32),
            vmem((2, QUAD, count, n_col * RANK), BF16),
            vmem((n_col, count, n_row * RANK), BF16),
            vmem((n_col, count, n_row * RANK), BF16),
            vmem((2, n_col, count, LANES), BF16),
            vmem((2, 2, n_col, count, LANES), BF16),
            vmem((n_row, count, n_col * RANK), BF16),
            vmem((2, n_row, count, n_col * RANK), BF16),
            vmem((2, 2, count, HALO * LEAF), BF16),
            vmem((3, 1, LANES), F32),
            vmem((2, n_col, 1, LANES), F32),
            vmem((total, 1, LANES), F32),
            dma((7,)),
            dma((2, 2)),
            dma((2, 2)),
            dma((2, 2, n_col)),
            dma((2, 2, n_col)),
            dma((2, n_row)),
            dma((2, n_row)),
            dma((2, n_col)),
            dma((2, n_col)),
            dma(()),
            dma(()),
        ],
        compiler_params=pltpu.CompilerParams(
            collective_id=0, has_side_effects=True, vmem_limit_bytes=34 * 1024 * 1024
        ),
        name="gmres",
    )(*(pltpu.with_memory_space_constraint(a, pltpu.HBM) for a in operands))
    return pl.pallas_call(
        finish,
        out_shape=(field, field),
        in_specs=[vmem_spec] * 4,
        out_specs=(hbm_spec,) * 2,
        scratch_shapes=[vmem((count, width), F32), vmem((count, width), F32), dma((CHUNKS, 2))],
        compiler_params=pltpu.CompilerParams(vmem_limit_bytes=16 * 1024 * 1024),
        name="combine",
    )(coef, rhs_v, x, y)


def solution(mesh):
    in_specs = (
        P(None, ("row", "col")),
        P(("row", "col"), None, None),
        P(("row", "col"), None),
        P(("row", "col"), None),
        P("row", "col", None, None),
        P("row", "col", None, None),
        P(("row", "col"), None),
    )
    out_specs = (P(None, ("row", "col")), P(None, ("row", "col")))
    return jax.shard_map(body, mesh=mesh, in_specs=in_specs, out_specs=out_specs, check_vma=False)
```

```python
import jax
import jax.numpy as jnp
from jax import lax
from jax.experimental import pallas as pl
from jax.experimental.pallas import tpu as pltpu
from jax.sharding import PartitionSpec as P

LEAF = 64
RANK = 32
HALO = 4
LANES = 128
QUAD = LANES // RANK
PAIRS_STEP = 16
PREPARE_STEP = 32
RING = 4
BF16 = jnp.bfloat16
F32 = jnp.float32
MESH = pl.DeviceIdType.MESH


def iota(shape, dim):
    return lax.broadcasted_iota(jnp.int32, shape, dim)


def dot(a, b):
    return jnp.dot(a, b, preferred_element_type=F32)


def dot_t(a, b):
    return lax.dot_general(a, b, (((1,), (1,)), ((), ())), preferred_element_type=F32)


def lanes_at(index, width):
    return pl.ds(pl.multiple_of(index * width, width), width)


def regroup(tiles, group):
    out = []
    for j in range(QUAD):
        made = None
        for c in range(QUAD):
            shift = (c - j) * RANK % LANES
            moved = pltpu.roll(tiles[c], shift, 1) if shift else tiles[c]
            made = moved if made is None else jnp.where(group == c, moved, made)
        out.append(made)
    return out


def tree(parts):
    while len(parts) > 1:
        parts = [parts[i] + parts[i + 1] for i in range(0, len(parts), 2)]
    return parts[0]


def kernel(
    offs_h, rhs_h, near_h, v_h, mixc_h, mixr_h, u_h, rhs, x, y, coef,
    offs, near_raw, v_raw, mixc, mixr, u_raw,
    near_w, v_big, u_big, pick_near, pick_v, pick_u,
    rim, xdup, nacc, left_c, left_r, right, z_mid, z_mix, z_near,
    zbuf, zrecv, tbuf, trecv, halo, part, early, sums,
    load_sem, halo_s, halo_r, z_s, z_r, t_s, t_r, early_s, early_r, sum_s, sum_r,
):
    n_row = lax.axis_size("row")
    n_col = lax.axis_size("col")
    total = n_row * n_col
    row = lax.axis_index("row")
    col = lax.axis_index("col")
    me = row * n_col + col
    count, width = rhs.shape
    leaves = width // LEAF
    nnear = offs.shape[0]
    slots = leaves // n_col
    tiles = slots // QUAD

    loads = {}
    for at, (name, src, dst) in enumerate(
        (("v", v_h, v_raw), ("rhs", rhs_h, rhs), ("offs", offs_h, offs), ("near", near_h, near_raw),
         ("mixc", mixc_h, mixc), ("u", u_h, u_raw), ("mixr", mixr_h, mixr))
    ):
        loads[name] = pltpu.make_async_copy(src, dst, load_sem.at[at])
        if name in ("v", "rhs", "offs"):
            loads[name].start()

    barrier = pltpu.get_barrier_semaphore()
    before = lax.rem(me + total - 1, total)
    after = lax.rem(me + 1, total)
    before_id = (before // n_col, lax.rem(before, n_col))
    after_id = (after // n_col, lax.rem(after, n_col))
    cores = n_row // RING
    place_x, place_core = row // cores, lax.rem(row, cores)
    place_z, place_y = col // RING, lax.rem(col, RING)

    def turn(base, by, size):
        return lax.rem(base + by, size) if by else base

    def away(by):
        return min(by, RING - by)

    rows = [turn(place_x, i // cores, RING) * cores + turn(place_core, i % cores, cores) for i in range(n_row)]
    cols = [turn(place_z, j // RING, RING) * RING + turn(place_y, j % RING, RING) for j in range(n_col)]

    def row_slot(r):
        dx = lax.rem(place_x + RING - r // cores, RING)
        return dx * cores + lax.rem(place_core + cores - r % cores, cores)

    def col_slot(c):
        dz = lax.rem(place_z + RING - c // RING, RING)
        return dz * RING + lax.rem(place_y + RING - c % RING, RING)

    row_far = [2 * away(i // cores) + i % cores for i in range(n_row)]
    col_far = [2 * (away(j // RING) + away(j % RING)) for j in range(n_col)]
    odd = lax.rem(place_x, 2)
    halves = (1 - place_x // 2, place_x // 2)
    targets = (
        ((2, 0), (2, 1), (3 - 2 * odd, 0), (3 - 2 * odd, 1)),
        ((1 + 2 * odd, 0), (1 + 2 * odd, 1), (0, 1), (None, 0)),
    )
    row_order = sorted(range(1, n_row), key=lambda i: -row_far[i])
    col_order = sorted(range(1, n_col), key=lambda j: -col_far[j])
    others = [(i, j) for i in range(n_row) for j in range(n_col) if i or j]
    others.sort(key=lambda p: -(row_far[p[0]] + col_far[p[1]]))

    greeted = [(row, cols[j]) for j in col_order] + [after_id, before_id] + [(rows[i], col) for i in row_order]
    for peer in greeted:
        pl.semaphore_signal(barrier, inc=1, device_id=peer, device_id_type=MESH)

    lane = iota((count, LANES), 1)
    low = lane < LEAF
    group = lane // RANK

    shape = (256, 256)
    r = iota(shape, 0)
    c = iota(shape, 1)
    same = (c % 16 == r // 16) & (c // 16 % 4 == r // 4 % 4)
    pick_v[...] = jnp.where(same & (c // 64 == (r // 16 + 4 - r % 4) % 4), 1.0, 0.0).astype(BF16)
    same = (c % 16 == r // 16) & (c // 16 % 8 == r // 2 % 8)
    pick_u[...] = jnp.where(same & (c // 128 == (r // 16 + r) % 2), 1.0, 0.0).astype(BF16)
    shape = (LANES, 256)
    r = iota(shape, 0)
    c = iota(shape, 1)
    b = c % nnear
    same = (c % LANES // nnear == r % LEAF // 2) & (b // 2 == r // LEAF)
    pick_near[...] = jnp.where(same & (c // LANES == (r + b) % 2), 1.0, 0.0).astype(BF16)

    def turned(tile, shift):
        return pltpu.roll(tile, shift, 1) if shift else tile

    def prepare_v():
        lane16 = iota((16, LANES), 1) // RANK
        place = lane16 == iota((16, LANES), 0) % QUAD
        blank = jnp.zeros((16, LANES), BF16)
        for b in range(leaves // 32):
            sides = []
            for h in range(2):
                base = b * 32 + h * 16
                raw = [v_raw[base:base + 16, t * LANES:(t + 1) * LANES] for t in range(16)]
                sides.append(
                    [[jnp.where(place, turned(a, d * RANK), blank) for a in raw] for d in range(4)]
                )
            for q in range(4):
                both = jnp.concatenate(
                    [
                        jnp.concatenate([s[d][4 * q + t] for d in range(4) for t in range(4)], axis=0)
                        for s in sides
                    ],
                    axis=1,
                )
                made = dot(pick_v[...], both)
                for h in range(2):
                    for i in range(16):
                        at = (b * 32 + h * 16 + i) * LEAF + q * 16
                        v_big[at:at + 16, :] = made[i * 16:(i + 1) * 16, h * LANES:(h + 1) * LANES].astype(BF16)

    def prepare_u():
        lane16 = iota((16, LANES), 1) // LEAF
        place = lane16 == iota((16, LANES), 0) % 2
        blank = jnp.zeros((16, LANES), BF16)
        for b in range(leaves // 32):
            sides = []
            for h in range(2):
                base = b * 32 + h * 16
                raw = [u_raw[base:base + 16, t * LANES:(t + 1) * LANES] for t in range(16)]
                sides.append(
                    [[jnp.where(place, turned(a, d * LEAF), blank) for a in raw] for d in range(2)]
                )
            for q in range(2):
                both = jnp.concatenate(
                    [
                        jnp.concatenate([s[d][8 * q + t] for d in range(2) for t in range(8)], axis=0)
                        for s in sides
                    ],
                    axis=1,
                )
                made = dot(pick_u[...], both)
                for h in range(2):
                    for i in range(16):
                        at = (b * 32 + h * 16 + i) * RANK + q * 16
                        side = i % QUAD // 2
                        tile = made[i * 16:(i + 1) * 16, h * LANES:(h + 1) * LANES].astype(BF16)
                        u_big[at:at + 16, side * LANES:(side + 1) * LANES] = tile
                        u_big[at:at + 16, (1 - side) * LANES:(2 - side) * LANES] = blank

    def prepare_near():
        size = nnear * LEAF // 2
        keep = (iota((size, LANES), 1) // LEAF) == iota((size, LANES), 0) % 2

        def block(b, carry):
            for k in range(PREPARE_STEP):
                pair = b * PREPARE_STEP + k
                sides = []
                for h in range(2):
                    raw = near_raw[lanes_at(pair * 2 + h, size), :].astype(F32)
                    sides.append(
                        jnp.concatenate(
                            [
                                jnp.where(keep, raw, 0.0).astype(BF16),
                                jnp.where(keep, pltpu.roll(raw, LEAF, 1), 0.0).astype(BF16),
                            ],
                            axis=0,
                        )
                    )
                made = dot(pick_near[...], jnp.concatenate(sides, axis=1))
                for h in range(2):
                    for m in range(nnear // 2):
                        near_w[lanes_at(pair * 2 + h, LEAF), m * LANES:(m + 1) * LANES] = made[
                            m * LEAF:(m + 1) * LEAF, h * LANES:(h + 1) * LANES
                        ].astype(BF16)
            return carry

        lax.fori_loop(0, leaves // 2 // PREPARE_STEP, block, 0)

    def spread(tile, first):
        swapped = pltpu.roll(tile, LEAF, 1)
        xdup[first] = jnp.where(low, tile, swapped)
        xdup[first + 1] = jnp.where(low, swapped, tile)

    def remote(src, dst, send, recv, to):
        return pltpu.make_async_remote_copy(
            src_ref=src, dst_ref=dst, send_sem=send, recv_sem=recv, device_id=to, device_id_type=MESH
        )

    def line_of(accs):
        spot = lane - iota((count, LANES), 0)
        spread_out = jnp.zeros((count, LANES), F32)
        for k, acc in enumerate(accs):
            spread_out = jnp.where(spot == k * count, jnp.sum(acc, axis=1, keepdims=True), spread_out)
        return jnp.sum(spread_out, axis=0, keepdims=True)

    def columns_of(line, many):
        spot = lane - iota((count, LANES), 0)
        return [jnp.sum(jnp.where(spot == k * count, line, 0.0), axis=1, keepdims=True) for k in range(many)]

    def group_copy(at, s):
        to = (rows[s], col) if at == 0 else (row, cols[s])
        return remote(part.at[at], early.at[at, s], early_s.at[at, s], early_r.at[at, s], to)

    def group_start(at, line):
        part[at] = line
        early[at, 0] = line
        for s in (row_order, col_order)[at]:
            group_copy(at, s).start()

    def group_finish(at):
        for s in (row_order, col_order)[at]:
            group_copy(at, s).wait()
        return tree([early[at, d] for d in range((n_row, n_col)[at])])

    def sum_start(line):
        part[2] = line
        sums[0] = line
        for i, j in others:
            remote(part.at[2], sums.at[i * n_col + j], sum_s, sum_r, (rows[i], cols[j])).start()

    def sum_finish():
        everything = remote(sums.at[1:total], sums.at[1:total], sum_s, sum_r, (row, cols[1]))
        everything.wait_send()
        everything.wait_recv()
        return tree([sums[d] for d in range(total)])

    def prepare_z():
        blank = jnp.zeros((LANES, LANES), BF16)

        for at4 in range(leaves // QUAD):
            p, tt = at4 // tiles, at4 % tiles
            made = dot(u_big[at4 * LANES:(at4 + 1) * LANES, :], v_big[at4 * 256:(at4 + 1) * 256, :]).astype(BF16)
            rows_of = slice(tt * LANES, (tt + 1) * LANES)
            z_mid[p, rows_of, rows_of] = made
            z_mid[p, rows_of, (1 - tt) * LANES:(2 - tt) * LANES] = blank
        for p in range(n_col):
            made = dot(mixr[p], z_mid[p]).astype(BF16)
            for tt in range(tiles):
                z_mix[tt, p] = made[:, tt * LANES:(tt + 1) * LANES]

    def near_z():
        for g4 in range(leaves // QUAD):
            made = nacc[:, g4 * 256:(g4 + 1) * 256].astype(BF16)
            z_near[g4] = dot(made, v_big[g4 * 256:(g4 + 1) * 256, :])

    def z_mixed(h):
        for s in col_order + [0]:
            z = dot(left_r[cols[s]], z_mix[halves[h], cols[s]]) + z_near[cols[s] * tiles + halves[h]]
            if s:
                zbuf[h, cols[s]] = z.astype(BF16)
            else:
                zrecv[1, h, 0] = z.astype(BF16)

    def z_pass(at, h, field):
        for s in col_order + [0]:
            at4 = cols[s] * tiles + halves[h]
            made = jnp.concatenate(
                [field[:, lanes_at(at4 * 2 + k, LANES)].astype(BF16) for k in range(2)], axis=1
            )
            z = dot(made, v_big[lanes_at(at4, 256), :]).astype(BF16)
            if s:
                zbuf[h, cols[s]] = z
            else:
                zrecv[at, h, 0] = z

    def z_copy(at, h, s):
        return remote(
            zbuf.at[h, cols[s]], zrecv.at[at, h, s], z_s.at[at, h, s], z_r.at[at, h, s], (row, cols[s])
        )

    def t_copy(at, s, to):
        return remote(tbuf.at[to], trecv.at[at, s], t_s.at[at, s], t_r.at[at, s], (to, col))

    def halo_copy(at, side):
        return remote(rim.at[at, side], halo.at[at, side], halo_s.at[at, side], halo_r.at[at, side], (after_id, before_id)[side])

    def near(b, carry):
        for k in range(PAIRS_STEP):
            pair = b * PAIRS_STEP + k
            lefts = []
            for h in range(2):
                leaf = pair * 2 + h
                picked = [xdup[leaf + HALO]] + [xdup[leaf + HALO + offs[n, leaf]] for n in range(1, nnear)]
                lefts.append(
                    jnp.concatenate(
                        [jnp.where(low, picked[2 * m], picked[2 * m + 1]) for m in range(nnear // 2)], axis=1
                    )
                )
            both = dot_t(jnp.concatenate(lefts, axis=0), near_w[lanes_at(pair, 2 * LEAF), :])
            nacc[:, lanes_at(pair, LANES)] = jnp.where(low, both[:count], both[count:])
        return carry

    steps = leaves // 2 // PAIRS_STEP

    def take(at, field, dots):
        accs = [jnp.zeros((count, LANES), F32) for _ in range(len(dots) + 1)]
        for t in range(width // LANES):
            where = slice(t * LANES, (t + 1) * LANES)
            tile = field[:, where]
            rounded = tile.astype(BF16)
            spread(rounded, HALO + 2 * t)
            for m, other in enumerate(dots):
                accs[m] = accs[m] + other[:, where] * tile
            accs[-1] = accs[-1] + tile * tile
            for side, k in ((0, t - width // LANES + HALO // 2), (1, t)):
                if 0 <= k < HALO // 2:
                    rim[at, side, :, k * LANES:(k + 1) * LANES] = rounded
        for side in range(2):
            halo_copy(at, side).start()
        return accs

    def operator(at, out):
        if at == 0:
            loads["near"].wait()
            prepare_near()
            loads["offs"].wait()
        lax.fori_loop(1, steps - 1, near, 0)
        if at == 0:
            loads["u"].wait()
            prepare_u()
        for h in range(2):
            for s in range(1, n_col):
                z_copy(at, h, s).wait()
            if at == 0 and h == 0:
                loads["mixc"].wait()
            for cq in range(n_col // QUAD):
                got = regroup([zrecv[at, h, col_slot(cq * QUAD + c4)] for c4 in range(QUAD)], group)
                for j4 in range(QUAD):
                    left_c[h, j4, :, cq * LANES:(cq + 1) * LANES] = got[j4]
            ready = []
            for dx, dc in targets[h]:
                if len(ready) == 2:
                    for s, to in ready:
                        t_copy(at, s, to).start()
                    ready = []
                to = lax.rem(place_x + (0 if dx is None else dx), RING) * cores + turn(place_core, dc, cores)
                made = dot(left_c[h, lax.rem(to, QUAD)], mixc[to]).astype(BF16)
                if dx is None:
                    trecv[at, 0] = made
                else:
                    tbuf[to] = made
                    ready.append((dx * cores + dc, to))
            for s, to in ready:
                t_copy(at, s, to).start()
        if at == 1:
            group_start(1, group_finish(0))
        if at == 0:
            loads["mixr"].wait()
            prepare_z()
        for side in range(2):
            halo_copy(at, side).wait()
        for side, beyond, first in ((0, me == 0, 0), (1, me == total - 1, leaves + HALO)):
            for k in range(HALO // 2):
                tile = halo[at, side, :, k * LANES:(k + 1) * LANES]
                spread(jnp.where(beyond, jnp.zeros_like(tile), tile), first + 2 * k)
        for b in (0, steps - 1):
            near(b, 0)
        if at == 0:
            near_z()
        for s in range(1, n_row):
            t_copy(at, s, rows[s]).wait()
        for pq in range(n_col // QUAD):
            for rq in range(n_row // QUAD):
                got = regroup(
                    [
                        trecv[at, row_slot(rq * QUAD + r4), :, pq * LANES:(pq + 1) * LANES]
                        for r4 in range(QUAD)
                    ],
                    group,
                )
                for p4 in range(QUAD):
                    left_r[pq * QUAD + p4, :, rq * LANES:(rq + 1) * LANES] = got[p4]
        if at == 0:
            for h in range(2):
                z_mixed(h)
                for s in col_order:
                    z_copy(1, h, s).start()
        for p in range(n_col):
            right[p] = dot(left_r[p], mixr[p]).astype(BF16)
        accs = [jnp.zeros((count, LANES), F32) for _ in range(3)]
        for p in range(n_col):
            for tt in range(tiles):
                at4 = p * tiles + tt
                far = dot(right[p, :, tt * LANES:(tt + 1) * LANES], u_big[at4 * LANES:(at4 + 1) * LANES, :])
                for k in range(2):
                    where = slice((at4 * 2 + k) * LANES, (at4 * 2 + k + 1) * LANES)
                    image = nacc[:, where] + far[:, k * LANES:(k + 1) * LANES]
                    if at == 1:
                        x_tile = x[:, where]
                        image = x_tile + image
                        for m, other in enumerate((rhs[:, where], x_tile, image)):
                            accs[m] = accs[m] + other * image
                    out[:, where] = image
        return accs

    loads["v"].wait()
    for name in ("near", "mixc", "u", "mixr"):
        loads[name].start()
    prepare_v()
    loads["rhs"].wait()
    for h in range(2):
        z_pass(0, h, rhs)
    pl.semaphore_wait(barrier, len(greeted))
    for h in range(2):
        for s in col_order:
            z_copy(0, h, s).start()
    norm = take(0, rhs, ())
    operator(0, x)
    first = take(1, x, (rhs,))
    early_line = line_of(norm + first)
    group_start(0, early_line)
    second = operator(1, y)
    sum_start(line_of(second))
    rr, rx, xx = columns_of(group_finish(1), 3)
    ry, xy, yy = columns_of(sum_finish(), 3)

    beta = jnp.sqrt(rr)
    d = rx / rr
    h11 = 1.0 + d
    rho_sq = xx - d * rx
    rho = jnp.sqrt(rho_sq)
    h21 = rho / beta
    h12 = (ry - d * (rr + rx)) / (beta * rho)
    across = xy - d * ry
    h22 = across / rho_sq - d
    h32 = jnp.sqrt((yy - ry * ry / rr - across * across / rho_sq) / rho_sq)
    m11 = h11 * h11 + h21 * h21
    m12 = h11 * h12 + h21 * h22
    m22 = h12 * h12 + h22 * h22 + h32 * h32
    det = m11 * m22 - m12 * m12
    y1 = (m22 * h11 - m12 * h12) / det
    y2 = beta * (m11 * h12 - m12 * h11) / det
    on_x = y2 / rho
    on_r = y1 - on_x * d
    coef[0] = jnp.broadcast_to(on_r, (count, LANES))
    coef[1] = jnp.broadcast_to(on_x, (count, LANES))


CHUNKS = 4


def finish(coef, rhs, x, y, sol_h, res_h, sol, res, sem):
    count, width = rhs.shape
    on_r = coef[0]
    on_x = coef[1]
    size = width // CHUNKS
    copies = []
    for c in range(CHUNKS):
        for t in range(size // LANES):
            where = slice(c * size + t * LANES, c * size + (t + 1) * LANES)
            r_tile = rhs[:, where]
            x_tile = x[:, where]
            sol[:, where] = on_r * r_tile + on_x * x_tile
            res[:, where] = r_tile - on_r * (r_tile + x_tile) - on_x * y[:, where]
        span = slice(c * size, (c + 1) * size)
        for k, (src, dst) in enumerate(((sol, sol_h), (res, res_h))):
            copies.append(pltpu.make_async_copy(src.at[:, span], dst.at[:, span], sem.at[c, k]))
            copies[-1].start()
    for copy in copies:
        copy.wait()


def body(rhs, near_blocks, near_offsets, v_factor, mix_col, mix_row, u_factor):
    n_row = lax.axis_size("row")
    n_col = lax.axis_size("col")
    count, width = rhs.shape
    leaves, nnear = near_offsets.shape
    pieces = near_blocks.shape[2] // LANES
    near_rows = (
        near_blocks.reshape(leaves, nnear, pieces, LANES).transpose(0, 2, 1, 3).reshape(leaves * pieces * nnear, LANES)
    )
    mixc = mix_col[0]
    mixr = mix_row[0]
    slots = leaves // n_col
    total = n_row * n_col
    operands = (near_offsets.T, rhs, near_rows, v_factor, mixc, mixr, u_factor)
    vmem = pltpu.VMEM
    dma = pltpu.SemaphoreType.DMA
    field = jax.ShapeDtypeStruct((count, width), F32)
    hbm_spec = pl.BlockSpec(memory_space=pltpu.HBM)
    vmem_spec = pl.BlockSpec(memory_space=pltpu.VMEM)
    rhs_v, x, y, coef = pl.pallas_call(
        kernel,
        out_shape=(field, field, field, jax.ShapeDtypeStruct((2, count, LANES), F32)),
        in_specs=[hbm_spec] * 7,
        out_specs=(vmem_spec,) * 4,
        scratch_shapes=[
            pltpu.SMEM((nnear, leaves), jnp.int32),
            vmem(near_rows.shape, BF16),
            vmem(v_factor.shape, BF16),
            vmem(mixc.shape, BF16),
            vmem(mixr.shape, BF16),
            vmem(u_factor.shape, BF16),
            vmem((leaves * LEAF, nnear * LEAF), BF16),
            vmem((leaves * LEAF, LANES), BF16),
            vmem((leaves * RANK, 2 * LANES), BF16),
            vmem((LANES, 256), BF16),
            vmem((256, 256), BF16),
            vmem((256, 256), BF16),
            vmem((2, 2, count, HALO * LEAF), BF16),
            vmem((leaves + 2 * HALO, count, LANES), BF16),
            vmem((count, width), F32),
            vmem((2, QUAD, count, n_col * RANK), BF16),
            vmem((n_col, count, n_row * RANK), BF16),
            vmem((n_col, count, n_row * RANK), BF16),
            vmem((n_col, 2 * LANES, 2 * LANES), BF16),
            vmem((2, n_col, 2 * LANES, LANES), BF16),
            vmem((leaves // QUAD, count, LANES), F32),
            vmem((2, n_col, count, LANES), BF16),
            vmem((2, 2, n_col, count, LANES), BF16),
            vmem((n_row, count, n_col * RANK), BF16),
            vmem((2, n_row, count, n_col * RANK), BF16),
            vmem((2, 2, count, HALO * LEAF), BF16),
            vmem((3, 1, LANES), F32),
            vmem((2, n_col, 1, LANES), F32),
            vmem((total, 1, LANES), F32),
            dma((7,)),
            dma((2, 2)),
            dma((2, 2)),
            dma((2, 2, n_col)),
            dma((2, 2, n_col)),
            dma((2, n_row)),
            dma((2, n_row)),
            dma((2, n_col)),
            dma((2, n_col)),
            dma(()),
            dma(()),
        ],
        compiler_params=pltpu.CompilerParams(
            collective_id=0, has_side_effects=True, vmem_limit_bytes=34 * 1024 * 1024
        ),
        name="gmres",
    )(*(pltpu.with_memory_space_constraint(a, pltpu.HBM) for a in operands))
    return pl.pallas_call(
        finish,
        out_shape=(field, field),
        in_specs=[vmem_spec] * 4,
        out_specs=(hbm_spec,) * 2,
        scratch_shapes=[vmem((count, width), F32), vmem((count, width), F32), dma((CHUNKS, 2))],
        compiler_params=pltpu.CompilerParams(vmem_limit_bytes=16 * 1024 * 1024),
        name="combine",
    )(coef, rhs_v, x, y)


def solution(mesh):
    in_specs = (
        P(None, ("row", "col")),
        P(("row", "col"), None, None),
        P(("row", "col"), None),
        P(("row", "col"), None),
        P("row", "col", None, None),
        P("row", "col", None, None),
        P(("row", "col"), None),
    )
    out_specs = (P(None, ("row", "col")), P(None, ("row", "col")))
    return jax.shard_map(body, mesh=mesh, in_specs=in_specs, out_specs=out_specs, check_vma=False)
```

```python
import jax
import jax.numpy as jnp
from jax import lax
from jax.experimental import pallas as pl
from jax.experimental.pallas import tpu as pltpu
from jax.sharding import PartitionSpec as P

LEAF = 64
RANK = 32
HALO = 4
LANES = 128
QUAD = LANES // RANK
PAIRS_STEP = 16
PREPARE_STEP = 32
RING = 4
BF16 = jnp.bfloat16
F32 = jnp.float32
MESH = pl.DeviceIdType.MESH


def iota(shape, dim):
    return lax.broadcasted_iota(jnp.int32, shape, dim)


def dot(a, b):
    return jnp.dot(a, b, preferred_element_type=F32)


def dot_t(a, b):
    return lax.dot_general(a, b, (((1,), (1,)), ((), ())), preferred_element_type=F32)


def lanes_at(index, width):
    return pl.ds(pl.multiple_of(index * width, width), width)


def regroup(tiles, group):
    out = []
    for j in range(QUAD):
        made = None
        for c in range(QUAD):
            shift = (c - j) * RANK % LANES
            moved = pltpu.roll(tiles[c], shift, 1) if shift else tiles[c]
            made = moved if made is None else jnp.where(group == c, moved, made)
        out.append(made)
    return out


def tree(parts):
    while len(parts) > 1:
        parts = [parts[i] + parts[i + 1] for i in range(0, len(parts), 2)]
    return parts[0]


def kernel(
    offs_h, rhs_h, near_h, v_h, mixc_h, mixr_h, u_h, rhs, x, y, coef,
    offs, near_raw, v_raw, mixc, mixr, u_raw,
    near_w, v_big, u_big, pick_near, pick_v, pick_u,
    rim, xdup, nacc, left_c, left_r, right, z_mid, z_mix, z_near,
    zbuf, zrecv, tbuf, trecv, halo, part, early, sums,
    load_sem, halo_s, halo_r, z_s, z_r, t_s, t_r, early_s, early_r, sum_s, sum_r,
):
    n_row = lax.axis_size("row")
    n_col = lax.axis_size("col")
    total = n_row * n_col
    row = lax.axis_index("row")
    col = lax.axis_index("col")
    me = row * n_col + col
    count, width = rhs.shape
    leaves = width // LEAF
    nnear = offs.shape[0]
    slots = leaves // n_col
    tiles = slots // QUAD

    loads = {}
    for at, (name, src, dst) in enumerate(
        (("v", v_h, v_raw), ("rhs", rhs_h, rhs), ("offs", offs_h, offs), ("near", near_h, near_raw),
         ("mixc", mixc_h, mixc), ("u", u_h, u_raw), ("mixr", mixr_h, mixr))
    ):
        loads[name] = pltpu.make_async_copy(src, dst, load_sem.at[at])
        if name in ("v", "rhs", "offs"):
            loads[name].start()

    barrier = pltpu.get_barrier_semaphore()
    before = lax.rem(me + total - 1, total)
    after = lax.rem(me + 1, total)
    before_id = (before // n_col, lax.rem(before, n_col))
    after_id = (after // n_col, lax.rem(after, n_col))
    cores = n_row // RING
    place_x, place_core = row // cores, lax.rem(row, cores)
    place_z, place_y = col // RING, lax.rem(col, RING)

    def turn(base, by, size):
        return lax.rem(base + by, size) if by else base

    def away(by):
        return min(by, RING - by)

    rows = [turn(place_x, i // cores, RING) * cores + turn(place_core, i % cores, cores) for i in range(n_row)]
    cols = [turn(place_z, j // RING, RING) * RING + turn(place_y, j % RING, RING) for j in range(n_col)]

    def row_slot(r):
        dx = lax.rem(place_x + RING - r // cores, RING)
        return dx * cores + lax.rem(place_core + cores - r % cores, cores)

    def col_slot(c):
        dz = lax.rem(place_z + RING - c // RING, RING)
        return dz * RING + lax.rem(place_y + RING - c % RING, RING)

    row_far = [2 * away(i // cores) + i % cores for i in range(n_row)]
    col_far = [2 * (away(j // RING) + away(j % RING)) for j in range(n_col)]
    odd = lax.rem(place_x, 2)
    halves = (1 - place_x // 2, place_x // 2)
    targets = (
        ((2, 0), (2, 1), (3 - 2 * odd, 0), (3 - 2 * odd, 1)),
        ((1 + 2 * odd, 0), (1 + 2 * odd, 1), (0, 1), (None, 0)),
    )
    row_order = sorted(range(1, n_row), key=lambda i: -row_far[i])
    col_order = sorted(range(1, n_col), key=lambda j: -col_far[j])
    others = [(i, j) for i in range(n_row) for j in range(n_col) if i or j]
    others.sort(key=lambda p: -(row_far[p[0]] + col_far[p[1]]))

    greeted = [(row, cols[j]) for j in col_order] + [after_id, before_id] + [(rows[i], col) for i in row_order]
    for peer in greeted:
        pl.semaphore_signal(barrier, inc=1, device_id=peer, device_id_type=MESH)

    lane = iota((count, LANES), 1)
    low = lane < LEAF
    group = lane // RANK

    shape = (256, 256)
    r = iota(shape, 0)
    c = iota(shape, 1)
    same = (c % 16 == r // 16) & (c // 16 % 4 == r // 4 % 4)
    pick_v[...] = jnp.where(same & (c // 64 == (r // 16 + 4 - r % 4) % 4), 1.0, 0.0).astype(BF16)
    same = (c % 16 == r // 16) & (c // 16 % 8 == r // 2 % 8)
    pick_u[...] = jnp.where(same & (c // 128 == (r // 16 + r) % 2), 1.0, 0.0).astype(BF16)
    shape = (LANES, 256)
    r = iota(shape, 0)
    c = iota(shape, 1)
    b = c % nnear
    same = (c % LANES // nnear == r % LEAF // 2) & (b // 2 == r // LEAF)
    pick_near[...] = jnp.where(same & (c // LANES == (r + b) % 2), 1.0, 0.0).astype(BF16)

    def turned(tile, shift):
        return pltpu.roll(tile, shift, 1) if shift else tile

    def prepare_v():
        lane16 = iota((16, LANES), 1) // RANK
        place = lane16 == iota((16, LANES), 0) % QUAD
        blank = jnp.zeros((16, LANES), BF16)
        for b in range(leaves // 32):
            sides = []
            for h in range(2):
                base = b * 32 + h * 16
                raw = [v_raw[base:base + 16, t * LANES:(t + 1) * LANES] for t in range(16)]
                sides.append(
                    [[jnp.where(place, turned(a, d * RANK), blank) for a in raw] for d in range(4)]
                )
            for q in range(4):
                both = jnp.concatenate(
                    [
                        jnp.concatenate([s[d][4 * q + t] for d in range(4) for t in range(4)], axis=0)
                        for s in sides
                    ],
                    axis=1,
                )
                made = dot(pick_v[...], both)
                for h in range(2):
                    for i in range(16):
                        at = (b * 32 + h * 16 + i) * LEAF + q * 16
                        v_big[at:at + 16, :] = made[i * 16:(i + 1) * 16, h * LANES:(h + 1) * LANES].astype(BF16)

    def prepare_u():
        lane16 = iota((16, LANES), 1) // LEAF
        place = lane16 == iota((16, LANES), 0) % 2
        blank = jnp.zeros((16, LANES), BF16)
        for b in range(leaves // 32):
            sides = []
            for h in range(2):
                base = b * 32 + h * 16
                raw = [u_raw[base:base + 16, t * LANES:(t + 1) * LANES] for t in range(16)]
                sides.append(
                    [[jnp.where(place, turned(a, d * LEAF), blank) for a in raw] for d in range(2)]
                )
            for q in range(2):
                both = jnp.concatenate(
                    [
                        jnp.concatenate([s[d][8 * q + t] for d in range(2) for t in range(8)], axis=0)
                        for s in sides
                    ],
                    axis=1,
                )
                made = dot(pick_u[...], both)
                for h in range(2):
                    for i in range(16):
                        at = (b * 32 + h * 16 + i) * RANK + q * 16
                        side = i % QUAD // 2
                        tile = made[i * 16:(i + 1) * 16, h * LANES:(h + 1) * LANES].astype(BF16)
                        u_big[at:at + 16, side * LANES:(side + 1) * LANES] = tile
                        u_big[at:at + 16, (1 - side) * LANES:(2 - side) * LANES] = blank

    def prepare_near():
        size = nnear * LEAF // 2
        keep = (iota((size, LANES), 1) // LEAF) == iota((size, LANES), 0) % 2

        def block(b, carry):
            for k in range(PREPARE_STEP):
                pair = b * PREPARE_STEP + k
                sides = []
                for h in range(2):
                    raw = near_raw[lanes_at(pair * 2 + h, size), :].astype(F32)
                    sides.append(
                        jnp.concatenate(
                            [
                                jnp.where(keep, raw, 0.0).astype(BF16),
                                jnp.where(keep, pltpu.roll(raw, LEAF, 1), 0.0).astype(BF16),
                            ],
                            axis=0,
                        )
                    )
                made = dot(pick_near[...], jnp.concatenate(sides, axis=1))
                for h in range(2):
                    for m in range(nnear // 2):
                        near_w[lanes_at(pair * 2 + h, LEAF), m * LANES:(m + 1) * LANES] = made[
                            m * LEAF:(m + 1) * LEAF, h * LANES:(h + 1) * LANES
                        ].astype(BF16)
            return carry

        lax.fori_loop(0, leaves // 2 // PREPARE_STEP, block, 0)

    def spread(tile, first):
        swapped = pltpu.roll(tile, LEAF, 1)
        xdup[first] = jnp.where(low, tile, swapped)
        xdup[first + 1] = jnp.where(low, swapped, tile)

    def remote(src, dst, send, recv, to):
        return pltpu.make_async_remote_copy(
            src_ref=src, dst_ref=dst, send_sem=send, recv_sem=recv, device_id=to, device_id_type=MESH
        )

    def line_of(accs):
        spot = lane - iota((count, LANES), 0)
        spread_out = jnp.zeros((count, LANES), F32)
        for k, acc in enumerate(accs):
            spread_out = jnp.where(spot == k * count, jnp.sum(acc, axis=1, keepdims=True), spread_out)
        return jnp.sum(spread_out, axis=0, keepdims=True)

    def columns_of(line, many):
        spot = lane - iota((count, LANES), 0)
        return [jnp.sum(jnp.where(spot == k * count, line, 0.0), axis=1, keepdims=True) for k in range(many)]

    def group_copy(at, s):
        to = (rows[s], col) if at == 0 else (row, cols[s])
        return remote(part.at[at], early.at[at, s], early_s.at[at, s], early_r.at[at, s], to)

    def group_start(at, line):
        part[at] = line
        early[at, 0] = line
        for s in (row_order, col_order)[at]:
            group_copy(at, s).start()

    def group_finish(at):
        for s in (row_order, col_order)[at]:
            group_copy(at, s).wait()
        return tree([early[at, d] for d in range((n_row, n_col)[at])])

    def sum_start(line):
        part[2] = line
        sums[0] = line
        for i, j in others:
            remote(part.at[2], sums.at[i * n_col + j], sum_s, sum_r, (rows[i], cols[j])).start()

    def sum_finish():
        everything = remote(sums.at[1:total], sums.at[1:total], sum_s, sum_r, (row, cols[1]))
        everything.wait_send()
        everything.wait_recv()
        return tree([sums[d] for d in range(total)])

    def prepare_z():
        blank = jnp.zeros((LANES, LANES), BF16)

        for at4 in range(leaves // QUAD):
            p, tt = at4 // tiles, at4 % tiles
            made = dot(u_big[at4 * LANES:(at4 + 1) * LANES, :], v_big[at4 * 256:(at4 + 1) * 256, :]).astype(BF16)
            rows_of = slice(tt * LANES, (tt + 1) * LANES)
            z_mid[p, rows_of, rows_of] = made
            z_mid[p, rows_of, (1 - tt) * LANES:(2 - tt) * LANES] = blank
        for p in range(n_col):
            made = dot(mixr[p], z_mid[p]).astype(BF16)
            for tt in range(tiles):
                z_mix[tt, p] = made[:, tt * LANES:(tt + 1) * LANES]

    def near_z():
        for g4 in range(leaves // QUAD):
            made = nacc[:, g4 * 256:(g4 + 1) * 256].astype(BF16)
            z_near[g4] = dot(made, v_big[g4 * 256:(g4 + 1) * 256, :])

    def z_mixed(h):
        for s in col_order + [0]:
            z = dot(left_r[cols[s]], z_mix[halves[h], cols[s]]) + z_near[cols[s] * tiles + halves[h]]
            if s:
                zbuf[h, cols[s]] = z.astype(BF16)
            else:
                zrecv[1, h, 0] = z.astype(BF16)

    def z_pass(at, h, field):
        for s in col_order + [0]:
            at4 = cols[s] * tiles + halves[h]
            made = jnp.concatenate(
                [field[:, lanes_at(at4 * 2 + k, LANES)].astype(BF16) for k in range(2)], axis=1
            )
            z = dot(made, v_big[lanes_at(at4, 256), :]).astype(BF16)
            if s:
                zbuf[h, cols[s]] = z
            else:
                zrecv[at, h, 0] = z

    def z_copy(at, h, s):
        return remote(
            zbuf.at[h, cols[s]], zrecv.at[at, h, s], z_s.at[at, h, s], z_r.at[at, h, s], (row, cols[s])
        )

    def t_copy(at, s, to):
        return remote(tbuf.at[to], trecv.at[at, s], t_s.at[at, s], t_r.at[at, s], (to, col))

    def halo_copy(at, side):
        return remote(rim.at[at, side], halo.at[at, side], halo_s.at[at, side], halo_r.at[at, side], (after_id, before_id)[side])

    def near(b, carry):
        for k in range(PAIRS_STEP):
            pair = b * PAIRS_STEP + k
            lefts = []
            for h in range(2):
                leaf = pair * 2 + h
                picked = [xdup[leaf + HALO]] + [xdup[leaf + HALO + offs[n, leaf]] for n in range(1, nnear)]
                lefts.append(
                    jnp.concatenate(
                        [jnp.where(low, picked[2 * m], picked[2 * m + 1]) for m in range(nnear // 2)], axis=1
                    )
                )
            both = dot_t(jnp.concatenate(lefts, axis=0), near_w[lanes_at(pair, 2 * LEAF), :])
            nacc[:, lanes_at(pair, LANES)] = jnp.where(low, both[:count], both[count:])
        return carry

    steps = leaves // 2 // PAIRS_STEP

    def take(at, field, dots):
        accs = [jnp.zeros((count, LANES), F32) for _ in range(len(dots) + 1)]
        for t in range(width // LANES):
            where = slice(t * LANES, (t + 1) * LANES)
            tile = field[:, where]
            rounded = tile.astype(BF16)
            spread(rounded, HALO + 2 * t)
            for m, other in enumerate(dots):
                accs[m] = accs[m] + other[:, where] * tile
            accs[-1] = accs[-1] + tile * tile
            for side, k in ((0, t - width // LANES + HALO // 2), (1, t)):
                if 0 <= k < HALO // 2:
                    rim[at, side, :, k * LANES:(k + 1) * LANES] = rounded
        for side in range(2):
            halo_copy(at, side).start()
        return accs

    def operator(at, out):
        if at == 0:
            loads["near"].wait()
            prepare_near()
            loads["offs"].wait()
        lax.fori_loop(1, steps - 1, near, 0)
        if at == 0:
            loads["u"].wait()
            prepare_u()
        for h in range(2):
            for s in range(1, n_col):
                z_copy(at, h, s).wait()
            if at == 0 and h == 0:
                loads["mixc"].wait()
            for cq in range(n_col // QUAD):
                got = regroup([zrecv[at, h, col_slot(cq * QUAD + c4)] for c4 in range(QUAD)], group)
                for j4 in range(QUAD):
                    left_c[h, j4, :, cq * LANES:(cq + 1) * LANES] = got[j4]
            ready = []
            for dx, dc in targets[h]:
                if len(ready) == 2:
                    for s, to in ready:
                        t_copy(at, s, to).start()
                    ready = []
                to = lax.rem(place_x + (0 if dx is None else dx), RING) * cores + turn(place_core, dc, cores)
                made = dot(left_c[h, lax.rem(to, QUAD)], mixc[to]).astype(BF16)
                if dx is None:
                    trecv[at, 0] = made
                else:
                    tbuf[to] = made
                    ready.append((dx * cores + dc, to))
            for s, to in ready:
                t_copy(at, s, to).start()
        if at == 1:
            group_start(1, group_finish(0))
        if at == 0:
            loads["mixr"].wait()
            prepare_z()
        for side in range(2):
            halo_copy(at, side).wait()
        for side, beyond, first in ((0, me == 0, 0), (1, me == total - 1, leaves + HALO)):
            for k in range(HALO // 2):
                tile = halo[at, side, :, k * LANES:(k + 1) * LANES]
                spread(jnp.where(beyond, jnp.zeros_like(tile), tile), first + 2 * k)
        for b in (0, steps - 1):
            near(b, 0)
        if at == 0:
            near_z()
        for s in range(1, n_row):
            t_copy(at, s, rows[s]).wait()
        for pq in range(n_col // QUAD):
            for rq in range(n_row // QUAD):
                got = regroup(
                    [
                        trecv[at, row_slot(rq * QUAD + r4), :, pq * LANES:(pq + 1) * LANES]
                        for r4 in range(QUAD)
                    ],
                    group,
                )
                for p4 in range(QUAD):
                    left_r[pq * QUAD + p4, :, rq * LANES:(rq + 1) * LANES] = got[p4]
        if at == 0:
            for h in range(2):
                z_mixed(h)
                for s in col_order:
                    z_copy(1, h, s).start()
        for p in range(n_col):
            right[p] = dot(left_r[p], mixr[p]).astype(BF16)
        accs = [jnp.zeros((count, LANES), F32) for _ in range(3)]
        for p in range(n_col):
            for tt in range(tiles):
                at4 = p * tiles + tt
                far = dot(right[p, :, tt * LANES:(tt + 1) * LANES], u_big[at4 * LANES:(at4 + 1) * LANES, :])
                for k in range(2):
                    where = slice((at4 * 2 + k) * LANES, (at4 * 2 + k + 1) * LANES)
                    image = nacc[:, where] + far[:, k * LANES:(k + 1) * LANES]
                    if at == 1:
                        x_tile = x[:, where]
                        image = x_tile + image
                        for m, other in enumerate((rhs[:, where], x_tile, image)):
                            accs[m] = accs[m] + other * image
                    out[:, where] = image
        return accs

    loads["v"].wait()
    for name in ("near", "mixc", "u", "mixr"):
        loads[name].start()
    prepare_v()
    loads["rhs"].wait()
    for h in range(2):
        z_pass(0, h, rhs)
    pl.semaphore_wait(barrier, len(greeted))
    for h in range(2):
        for s in col_order:
            z_copy(0, h, s).start()
    norm = take(0, rhs, ())
    operator(0, x)
    first = take(1, x, (rhs,))
    early_line = line_of(norm + first)
    group_start(0, early_line)
    second = operator(1, y)
    sum_start(line_of(second))
    rr, rx, xx = columns_of(group_finish(1), 3)
    ry, xy, yy = columns_of(sum_finish(), 3)

    beta = jnp.sqrt(rr)
    d = rx / rr
    h11 = 1.0 + d
    rho_sq = xx - d * rx
    rho = jnp.sqrt(rho_sq)
    h21 = rho / beta
    h12 = (ry - d * (rr + rx)) / (beta * rho)
    across = xy - d * ry
    h22 = across / rho_sq - d
    h32 = jnp.sqrt((yy - ry * ry / rr - across * across / rho_sq) / rho_sq)
    m11 = h11 * h11 + h21 * h21
    m12 = h11 * h12 + h21 * h22
    m22 = h12 * h12 + h22 * h22 + h32 * h32
    det = m11 * m22 - m12 * m12
    y1 = (m22 * h11 - m12 * h12) / det
    y2 = beta * (m11 * h12 - m12 * h11) / det
    on_x = y2 / rho
    on_r = y1 - on_x * d
    coef[0] = jnp.broadcast_to(on_r, (count, LANES))
    coef[1] = jnp.broadcast_to(on_x, (count, LANES))


CHUNKS = (4, 12, 16, 16, 16)


def finish(coef, rhs, x, y, sol_h, res_h, sol, res, sem):
    count, width = rhs.shape
    on_r = coef[0]
    on_x = coef[1]
    copies = []
    for c, many in enumerate(CHUNKS):
        first = sum(CHUNKS[:c])
        for t in range(first, first + many):
            where = slice(t * LANES, (t + 1) * LANES)
            r_tile = rhs[:, where]
            x_tile = x[:, where]
            sol[:, where] = on_r * r_tile + on_x * x_tile
            res[:, where] = r_tile - on_r * (r_tile + x_tile) - on_x * y[:, where]
        span = slice(first * LANES, (first + many) * LANES)
        for k, (src, dst) in enumerate(((sol, sol_h), (res, res_h))):
            copies.append(pltpu.make_async_copy(src.at[:, span], dst.at[:, span], sem.at[c, k]))
            copies[-1].start()
    for copy in copies:
        copy.wait()


def body(rhs, near_blocks, near_offsets, v_factor, mix_col, mix_row, u_factor):
    n_row = lax.axis_size("row")
    n_col = lax.axis_size("col")
    count, width = rhs.shape
    leaves, nnear = near_offsets.shape
    pieces = near_blocks.shape[2] // LANES
    near_rows = (
        near_blocks.reshape(leaves, nnear, pieces, LANES).transpose(0, 2, 1, 3).reshape(leaves * pieces * nnear, LANES)
    )
    mixc = mix_col[0]
    mixr = mix_row[0]
    slots = leaves // n_col
    total = n_row * n_col
    operands = (near_offsets.T, rhs, near_rows, v_factor, mixc, mixr, u_factor)
    vmem = pltpu.VMEM
    dma = pltpu.SemaphoreType.DMA
    field = jax.ShapeDtypeStruct((count, width), F32)
    hbm_spec = pl.BlockSpec(memory_space=pltpu.HBM)
    vmem_spec = pl.BlockSpec(memory_space=pltpu.VMEM)
    rhs_v, x, y, coef = pl.pallas_call(
        kernel,
        out_shape=(field, field, field, jax.ShapeDtypeStruct((2, count, LANES), F32)),
        in_specs=[hbm_spec] * 7,
        out_specs=(vmem_spec,) * 4,
        scratch_shapes=[
            pltpu.SMEM((nnear, leaves), jnp.int32),
            vmem(near_rows.shape, BF16),
            vmem(v_factor.shape, BF16),
            vmem(mixc.shape, BF16),
            vmem(mixr.shape, BF16),
            vmem(u_factor.shape, BF16),
            vmem((leaves * LEAF, nnear * LEAF), BF16),
            vmem((leaves * LEAF, LANES), BF16),
            vmem((leaves * RANK, 2 * LANES), BF16),
            vmem((LANES, 256), BF16),
            vmem((256, 256), BF16),
            vmem((256, 256), BF16),
            vmem((2, 2, count, HALO * LEAF), BF16),
            vmem((leaves + 2 * HALO, count, LANES), BF16),
            vmem((count, width), F32),
            vmem((2, QUAD, count, n_col * RANK), BF16),
            vmem((n_col, count, n_row * RANK), BF16),
            vmem((n_col, count, n_row * RANK), BF16),
            vmem((n_col, 2 * LANES, 2 * LANES), BF16),
            vmem((2, n_col, 2 * LANES, LANES), BF16),
            vmem((leaves // QUAD, count, LANES), F32),
            vmem((2, n_col, count, LANES), BF16),
            vmem((2, 2, n_col, count, LANES), BF16),
            vmem((n_row, count, n_col * RANK), BF16),
            vmem((2, n_row, count, n_col * RANK), BF16),
            vmem((2, 2, count, HALO * LEAF), BF16),
            vmem((3, 1, LANES), F32),
            vmem((2, n_col, 1, LANES), F32),
            vmem((total, 1, LANES), F32),
            dma((7,)),
            dma((2, 2)),
            dma((2, 2)),
            dma((2, 2, n_col)),
            dma((2, 2, n_col)),
            dma((2, n_row)),
            dma((2, n_row)),
            dma((2, n_col)),
            dma((2, n_col)),
            dma(()),
            dma(()),
        ],
        compiler_params=pltpu.CompilerParams(
            collective_id=0, has_side_effects=True, vmem_limit_bytes=34 * 1024 * 1024
        ),
        name="gmres",
    )(*(pltpu.with_memory_space_constraint(a, pltpu.HBM) for a in operands))
    return pl.pallas_call(
        finish,
        out_shape=(field, field),
        in_specs=[vmem_spec] * 4,
        out_specs=(hbm_spec,) * 2,
        scratch_shapes=[vmem((count, width), F32), vmem((count, width), F32), dma((len(CHUNKS), 2))],
        compiler_params=pltpu.CompilerParams(vmem_limit_bytes=16 * 1024 * 1024),
        name="combine",
    )(coef, rhs_v, x, y)


def solution(mesh):
    in_specs = (
        P(None, ("row", "col")),
        P(("row", "col"), None, None),
        P(("row", "col"), None),
        P(("row", "col"), None),
        P("row", "col", None, None),
        P("row", "col", None, None),
        P(("row", "col"), None),
    )
    out_specs = (P(None, ("row", "col")), P(None, ("row", "col")))
    return jax.shard_map(body, mesh=mesh, in_specs=in_specs, out_specs=out_specs, check_vma=False)
```

```python
import jax
import jax.numpy as jnp
from jax import lax
from jax.experimental import pallas as pl
from jax.experimental.pallas import tpu as pltpu
from jax.sharding import PartitionSpec as P

LEAF = 64
RANK = 32
HALO = 4
LANES = 128
QUAD = LANES // RANK
PAIRS_STEP = 16
PREPARE_STEP = 32
RING = 4
BF16 = jnp.bfloat16
F32 = jnp.float32
MESH = pl.DeviceIdType.MESH


def iota(shape, dim):
    return lax.broadcasted_iota(jnp.int32, shape, dim)


def dot(a, b):
    return jnp.dot(a, b, preferred_element_type=F32)


def dot_t(a, b):
    return lax.dot_general(a, b, (((1,), (1,)), ((), ())), preferred_element_type=F32)


def lanes_at(index, width):
    return pl.ds(pl.multiple_of(index * width, width), width)


def regroup(tiles, group):
    out = []
    for j in range(QUAD):
        made = None
        for c in range(QUAD):
            shift = (c - j) * RANK % LANES
            moved = pltpu.roll(tiles[c], shift, 1) if shift else tiles[c]
            made = moved if made is None else jnp.where(group == c, moved, made)
        out.append(made)
    return out


def tree(parts):
    while len(parts) > 1:
        parts = [parts[i] + parts[i + 1] for i in range(0, len(parts), 2)]
    return parts[0]


def kernel(
    offs_h, rhs_h, near_h, v_h, mixc_h, mixr_h, u_h, rhs, x, y, coef,
    offs, near_raw, v_raw, mixc, mixr, u_raw,
    near_w, v_big, u_big, pick_near, pick_v, pick_u,
    rim, xdup, nacc, left_c, left_r, right, z_mid, z_mix, z_near,
    zbuf, zrecv, tbuf, trecv, halo, part, early, sums,
    load_sem, halo_s, halo_r, z_s, z_r, t_s, t_r, early_s, early_r, sum_s, sum_r,
):
    n_row = lax.axis_size("row")
    n_col = lax.axis_size("col")
    total = n_row * n_col
    row = lax.axis_index("row")
    col = lax.axis_index("col")
    me = row * n_col + col
    count, width = rhs.shape
    leaves = width // LEAF
    nnear = offs.shape[0]
    slots = leaves // n_col
    tiles = slots // QUAD

    loads = {}
    for at, (name, src, dst) in enumerate(
        (("v", v_h, v_raw), ("rhs", rhs_h, rhs), ("offs", offs_h, offs), ("near", near_h, near_raw),
         ("mixc", mixc_h, mixc), ("u", u_h, u_raw), ("mixr", mixr_h, mixr))
    ):
        loads[name] = pltpu.make_async_copy(src, dst, load_sem.at[at])
        if name in ("v", "rhs", "offs"):
            loads[name].start()

    barrier = pltpu.get_barrier_semaphore()
    before = lax.rem(me + total - 1, total)
    after = lax.rem(me + 1, total)
    before_id = (before // n_col, lax.rem(before, n_col))
    after_id = (after // n_col, lax.rem(after, n_col))
    cores = n_row // RING
    place_x, place_core = row // cores, lax.rem(row, cores)
    place_z, place_y = col // RING, lax.rem(col, RING)

    def turn(base, by, size):
        return lax.rem(base + by, size) if by else base

    def away(by):
        return min(by, RING - by)

    rows = [turn(place_x, i // cores, RING) * cores + turn(place_core, i % cores, cores) for i in range(n_row)]
    cols = [turn(place_z, j // RING, RING) * RING + turn(place_y, j % RING, RING) for j in range(n_col)]

    def row_slot(r):
        dx = lax.rem(place_x + RING - r // cores, RING)
        return dx * cores + lax.rem(place_core + cores - r % cores, cores)

    def col_slot(c):
        dz = lax.rem(place_z + RING - c // RING, RING)
        return dz * RING + lax.rem(place_y + RING - c % RING, RING)

    row_far = [2 * away(i // cores) + i % cores for i in range(n_row)]
    col_far = [2 * (away(j // RING) + away(j % RING)) for j in range(n_col)]
    odd = lax.rem(place_x, 2)
    halves = (1 - place_x // 2, place_x // 2)
    targets = (
        ((2, 0), (2, 1), (3 - 2 * odd, 0), (3 - 2 * odd, 1)),
        ((1 + 2 * odd, 0), (1 + 2 * odd, 1), (0, 1), (None, 0)),
    )
    row_order = sorted(range(1, n_row), key=lambda i: -row_far[i])
    col_order = sorted(range(1, n_col), key=lambda j: -col_far[j])
    others = [(i, j) for i in range(n_row) for j in range(n_col) if i or j]
    others.sort(key=lambda p: -(row_far[p[0]] + col_far[p[1]]))

    greeted = [(row, cols[j]) for j in col_order] + [after_id, before_id] + [(rows[i], col) for i in row_order]
    for peer in greeted:
        pl.semaphore_signal(barrier, inc=1, device_id=peer, device_id_type=MESH)

    lane = iota((count, LANES), 1)
    low = lane < LEAF
    group = lane // RANK

    shape = (256, 256)
    r = iota(shape, 0)
    c = iota(shape, 1)
    same = (c % 16 == r // 16) & (c // 16 % 4 == r // 4 % 4)
    pick_v[...] = jnp.where(same & (c // 64 == (r // 16 + 4 - r % 4) % 4), 1.0, 0.0).astype(BF16)
    same = (c % 16 == r // 16) & (c // 16 % 8 == r // 2 % 8)
    pick_u[...] = jnp.where(same & (c // 128 == (r // 16 + r) % 2), 1.0, 0.0).astype(BF16)
    shape = (LANES, 256)
    r = iota(shape, 0)
    c = iota(shape, 1)
    b = c % nnear
    same = (c % LANES // nnear == r % LEAF // 2) & (b // 2 == r // LEAF)
    pick_near[...] = jnp.where(same & (c // LANES == (r + b) % 2), 1.0, 0.0).astype(BF16)

    def turned(tile, shift):
        return pltpu.roll(tile, shift, 1) if shift else tile

    def prepare_v():
        lane16 = iota((16, LANES), 1) // RANK
        place = lane16 == iota((16, LANES), 0) % QUAD
        blank = jnp.zeros((16, LANES), BF16)
        for b in range(leaves // 32):
            sides = []
            for h in range(2):
                base = b * 32 + h * 16
                raw = [v_raw[base:base + 16, t * LANES:(t + 1) * LANES] for t in range(16)]
                sides.append(
                    [[jnp.where(place, turned(a, d * RANK), blank) for a in raw] for d in range(4)]
                )
            for q in range(4):
                both = jnp.concatenate(
                    [
                        jnp.concatenate([s[d][4 * q + t] for d in range(4) for t in range(4)], axis=0)
                        for s in sides
                    ],
                    axis=1,
                )
                made = dot(pick_v[...], both)
                for h in range(2):
                    for i in range(16):
                        at = (b * 32 + h * 16 + i) * LEAF + q * 16
                        v_big[at:at + 16, :] = made[i * 16:(i + 1) * 16, h * LANES:(h + 1) * LANES].astype(BF16)

    def prepare_u():
        lane16 = iota((16, LANES), 1) // LEAF
        place = lane16 == iota((16, LANES), 0) % 2
        blank = jnp.zeros((16, LANES), BF16)
        for b in range(leaves // 32):
            sides = []
            for h in range(2):
                base = b * 32 + h * 16
                raw = [u_raw[base:base + 16, t * LANES:(t + 1) * LANES] for t in range(16)]
                sides.append(
                    [[jnp.where(place, turned(a, d * LEAF), blank) for a in raw] for d in range(2)]
                )
            for q in range(2):
                both = jnp.concatenate(
                    [
                        jnp.concatenate([s[d][8 * q + t] for d in range(2) for t in range(8)], axis=0)
                        for s in sides
                    ],
                    axis=1,
                )
                made = dot(pick_u[...], both)
                for h in range(2):
                    for i in range(16):
                        at = (b * 32 + h * 16 + i) * RANK + q * 16
                        side = i % QUAD // 2
                        tile = made[i * 16:(i + 1) * 16, h * LANES:(h + 1) * LANES].astype(BF16)
                        u_big[at:at + 16, side * LANES:(side + 1) * LANES] = tile
                        u_big[at:at + 16, (1 - side) * LANES:(2 - side) * LANES] = blank

    def prepare_near():
        size = nnear * LEAF // 2
        keep = (iota((size, LANES), 1) // LEAF) == iota((size, LANES), 0) % 2

        def block(b, carry):
            for k in range(PREPARE_STEP):
                pair = b * PREPARE_STEP + k
                sides = []
                for h in range(2):
                    raw = near_raw[lanes_at(pair * 2 + h, size), :].astype(F32)
                    sides.append(
                        jnp.concatenate(
                            [
                                jnp.where(keep, raw, 0.0).astype(BF16),
                                jnp.where(keep, pltpu.roll(raw, LEAF, 1), 0.0).astype(BF16),
                            ],
                            axis=0,
                        )
                    )
                made = dot(pick_near[...], jnp.concatenate(sides, axis=1))
                for h in range(2):
                    for m in range(nnear // 2):
                        near_w[lanes_at(pair * 2 + h, LEAF), m * LANES:(m + 1) * LANES] = made[
                            m * LEAF:(m + 1) * LEAF, h * LANES:(h + 1) * LANES
                        ].astype(BF16)
            return carry

        lax.fori_loop(0, leaves // 2 // PREPARE_STEP, block, 0)

    def spread(tile, first):
        swapped = pltpu.roll(tile, LEAF, 1)
        xdup[first] = jnp.where(low, tile, swapped)
        xdup[first + 1] = jnp.where(low, swapped, tile)

    def remote(src, dst, send, recv, to):
        return pltpu.make_async_remote_copy(
            src_ref=src, dst_ref=dst, send_sem=send, recv_sem=recv, device_id=to, device_id_type=MESH
        )

    def line_of(accs):
        spot = lane - iota((count, LANES), 0)
        spread_out = jnp.zeros((count, LANES), F32)
        for k, acc in enumerate(accs):
            spread_out = jnp.where(spot == k * count, jnp.sum(acc, axis=1, keepdims=True), spread_out)
        return jnp.sum(spread_out, axis=0, keepdims=True)

    def columns_of(line, many):
        spot = lane - iota((count, LANES), 0)
        return [jnp.sum(jnp.where(spot == k * count, line, 0.0), axis=1, keepdims=True) for k in range(many)]

    def group_copy(at, s):
        to = (rows[s], col) if at == 0 else (row, cols[s])
        return remote(part.at[at], early.at[at, s], early_s.at[at, s], early_r.at[at, s], to)

    def group_start(at, line):
        part[at] = line
        early[at, 0] = line
        for s in (row_order, col_order)[at]:
            group_copy(at, s).start()

    def group_finish(at):
        for s in (row_order, col_order)[at]:
            group_copy(at, s).wait()
        return tree([early[at, d] for d in range((n_row, n_col)[at])])

    def sum_start(line):
        part[2] = line
        sums[0] = line
        for i, j in others:
            remote(part.at[2], sums.at[i * n_col + j], sum_s, sum_r, (rows[i], cols[j])).start()

    def sum_finish():
        everything = remote(sums.at[1:total], sums.at[1:total], sum_s, sum_r, (row, cols[1]))
        everything.wait_send()
        everything.wait_recv()
        return tree([sums[d] for d in range(total)])

    def prepare_z():
        blank = jnp.zeros((LANES, LANES), BF16)

        for at4 in range(leaves // QUAD):
            p, tt = at4 // tiles, at4 % tiles
            made = dot(u_big[at4 * LANES:(at4 + 1) * LANES, :], v_big[at4 * 256:(at4 + 1) * 256, :]).astype(BF16)
            rows_of = slice(tt * LANES, (tt + 1) * LANES)
            z_mid[p, rows_of, rows_of] = made
            z_mid[p, rows_of, (1 - tt) * LANES:(2 - tt) * LANES] = blank
        for p in range(n_col):
            made = dot(mixr[p], z_mid[p]).astype(BF16)
            for tt in range(tiles):
                z_mix[tt, p] = made[:, tt * LANES:(tt + 1) * LANES]

    def near_z():
        for g4 in range(leaves // QUAD):
            made = nacc[:, g4 * 256:(g4 + 1) * 256].astype(BF16)
            z_near[g4] = dot(made, v_big[g4 * 256:(g4 + 1) * 256, :])

    def z_mixed(h):
        for s in col_order + [0]:
            z = dot(left_r[cols[s]], z_mix[halves[h], cols[s]]) + z_near[cols[s] * tiles + halves[h]]
            if s:
                zbuf[h, cols[s]] = z.astype(BF16)
            else:
                zrecv[1, h, 0] = z.astype(BF16)

    def z_pass(at, h, field):
        for s in col_order + [0]:
            at4 = cols[s] * tiles + halves[h]
            made = jnp.concatenate(
                [field[:, lanes_at(at4 * 2 + k, LANES)].astype(BF16) for k in range(2)], axis=1
            )
            z = dot(made, v_big[lanes_at(at4, 256), :]).astype(BF16)
            if s:
                zbuf[h, cols[s]] = z
            else:
                zrecv[at, h, 0] = z

    def z_copy(at, h, s):
        return remote(
            zbuf.at[h, cols[s]], zrecv.at[at, h, s], z_s.at[at, h, s], z_r.at[at, h, s], (row, cols[s])
        )

    def t_copy(at, s, to):
        return remote(tbuf.at[to], trecv.at[at, s], t_s.at[at, s], t_r.at[at, s], (to, col))

    def halo_copy(at, side):
        return remote(rim.at[at, side], halo.at[at, side], halo_s.at[at, side], halo_r.at[at, side], (after_id, before_id)[side])

    def near(b, carry):
        for k in range(PAIRS_STEP):
            pair = b * PAIRS_STEP + k
            lefts = []
            for h in range(2):
                leaf = pair * 2 + h
                picked = [xdup[leaf + HALO]] + [xdup[leaf + HALO + offs[n, leaf]] for n in range(1, nnear)]
                lefts.append(
                    jnp.concatenate(
                        [jnp.where(low, picked[2 * m], picked[2 * m + 1]) for m in range(nnear // 2)], axis=1
                    )
                )
            both = dot_t(jnp.concatenate(lefts, axis=0), near_w[lanes_at(pair, 2 * LEAF), :])
            nacc[:, lanes_at(pair, LANES)] = jnp.where(low, both[:count], both[count:])
        return carry

    steps = leaves // 2 // PAIRS_STEP

    def take(at, field, dots):
        accs = [jnp.zeros((count, LANES), F32) for _ in range(len(dots) + 1)]
        for t in range(width // LANES):
            where = slice(t * LANES, (t + 1) * LANES)
            tile = field[:, where]
            rounded = tile.astype(BF16)
            spread(rounded, HALO + 2 * t)
            for m, other in enumerate(dots):
                accs[m] = accs[m] + other[:, where] * tile
            accs[-1] = accs[-1] + tile * tile
            for side, k in ((0, t - width // LANES + HALO // 2), (1, t)):
                if 0 <= k < HALO // 2:
                    rim[at, side, :, k * LANES:(k + 1) * LANES] = rounded
        for side in range(2):
            halo_copy(at, side).start()
        return accs

    def operator(at, out):
        if at == 0:
            loads["near"].wait()
            prepare_near()
            loads["offs"].wait()
        lax.fori_loop(1, steps - 1, near, 0)
        if at == 0:
            loads["u"].wait()
            prepare_u()
        for h in range(2):
            for dz in (0, 1, 3, 2):
                for dy in range(RING):
                    if dz or dy:
                        z_copy(at, h, dz * RING + dy).wait()
                plane = lax.rem(place_z + RING - dz, RING)
                slots_of = [dz * RING + lax.rem(place_y + RING - c4, RING) for c4 in range(QUAD)]
                got = regroup([zrecv[at, h, s] for s in slots_of], group)
                for j4 in range(QUAD):
                    left_c[h, j4, :, lanes_at(plane, LANES)] = got[j4]
            if at == 0 and h == 0:
                loads["mixc"].wait()
            ready = []
            for dx, dc in targets[h]:
                if len(ready) == 2:
                    for s, to in ready:
                        t_copy(at, s, to).start()
                    ready = []
                to = lax.rem(place_x + (0 if dx is None else dx), RING) * cores + turn(place_core, dc, cores)
                made = dot(left_c[h, lax.rem(to, QUAD)], mixc[to]).astype(BF16)
                if dx is None:
                    trecv[at, 0] = made
                else:
                    tbuf[to] = made
                    ready.append((dx * cores + dc, to))
            for s, to in ready:
                t_copy(at, s, to).start()
        if at == 1:
            group_start(1, group_finish(0))
        if at == 0:
            loads["mixr"].wait()
            prepare_z()
        for side in range(2):
            halo_copy(at, side).wait()
        for side, beyond, first in ((0, me == 0, 0), (1, me == total - 1, leaves + HALO)):
            for k in range(HALO // 2):
                tile = halo[at, side, :, k * LANES:(k + 1) * LANES]
                spread(jnp.where(beyond, jnp.zeros_like(tile), tile), first + 2 * k)
        for b in (0, steps - 1):
            near(b, 0)
        if at == 0:
            near_z()
        for s in range(1, n_row):
            t_copy(at, s, rows[s]).wait()
        for pq in range(n_col // QUAD):
            for rq in range(n_row // QUAD):
                got = regroup(
                    [
                        trecv[at, row_slot(rq * QUAD + r4), :, pq * LANES:(pq + 1) * LANES]
                        for r4 in range(QUAD)
                    ],
                    group,
                )
                for p4 in range(QUAD):
                    left_r[pq * QUAD + p4, :, rq * LANES:(rq + 1) * LANES] = got[p4]
        if at == 0:
            for h in range(2):
                z_mixed(h)
                for s in col_order:
                    z_copy(1, h, s).start()
        for p in range(n_col):
            right[p] = dot(left_r[p], mixr[p]).astype(BF16)
        accs = [jnp.zeros((count, LANES), F32) for _ in range(3)]
        for p in range(n_col):
            for tt in range(tiles):
                at4 = p * tiles + tt
                far = dot(right[p, :, tt * LANES:(tt + 1) * LANES], u_big[at4 * LANES:(at4 + 1) * LANES, :])
                for k in range(2):
                    where = slice((at4 * 2 + k) * LANES, (at4 * 2 + k + 1) * LANES)
                    image = nacc[:, where] + far[:, k * LANES:(k + 1) * LANES]
                    if at == 1:
                        x_tile = x[:, where]
                        image = x_tile + image
                        for m, other in enumerate((rhs[:, where], x_tile, image)):
                            accs[m] = accs[m] + other * image
                    out[:, where] = image
        return accs

    loads["v"].wait()
    for name in ("near", "mixc", "u", "mixr"):
        loads[name].start()
    prepare_v()
    loads["rhs"].wait()
    for h in range(2):
        z_pass(0, h, rhs)
    pl.semaphore_wait(barrier, len(greeted))
    for h in range(2):
        for s in col_order:
            z_copy(0, h, s).start()
    norm = take(0, rhs, ())
    operator(0, x)
    first = take(1, x, (rhs,))
    early_line = line_of(norm + first)
    group_start(0, early_line)
    second = operator(1, y)
    sum_start(line_of(second))
    rr, rx, xx = columns_of(group_finish(1), 3)
    ry, xy, yy = columns_of(sum_finish(), 3)

    beta = jnp.sqrt(rr)
    d = rx / rr
    h11 = 1.0 + d
    rho_sq = xx - d * rx
    rho = jnp.sqrt(rho_sq)
    h21 = rho / beta
    h12 = (ry - d * (rr + rx)) / (beta * rho)
    across = xy - d * ry
    h22 = across / rho_sq - d
    h32 = jnp.sqrt((yy - ry * ry / rr - across * across / rho_sq) / rho_sq)
    m11 = h11 * h11 + h21 * h21
    m12 = h11 * h12 + h21 * h22
    m22 = h12 * h12 + h22 * h22 + h32 * h32
    det = m11 * m22 - m12 * m12
    y1 = (m22 * h11 - m12 * h12) / det
    y2 = beta * (m11 * h12 - m12 * h11) / det
    on_x = y2 / rho
    on_r = y1 - on_x * d
    coef[0] = jnp.broadcast_to(on_r, (count, LANES))
    coef[1] = jnp.broadcast_to(on_x, (count, LANES))


CHUNKS = (4, 12, 16, 16, 16)


def finish(coef, rhs, x, y, sol_h, res_h, sol, res, sem):
    count, width = rhs.shape
    on_r = coef[0]
    on_x = coef[1]
    copies = []
    for c, many in enumerate(CHUNKS):
        first = sum(CHUNKS[:c])
        for t in range(first, first + many):
            where = slice(t * LANES, (t + 1) * LANES)
            r_tile = rhs[:, where]
            x_tile = x[:, where]
            sol[:, where] = on_r * r_tile + on_x * x_tile
            res[:, where] = r_tile - on_r * (r_tile + x_tile) - on_x * y[:, where]
        span = slice(first * LANES, (first + many) * LANES)
        for k, (src, dst) in enumerate(((sol, sol_h), (res, res_h))):
            copies.append(pltpu.make_async_copy(src.at[:, span], dst.at[:, span], sem.at[c, k]))
            copies[-1].start()
    for copy in copies:
        copy.wait()


def body(rhs, near_blocks, near_offsets, v_factor, mix_col, mix_row, u_factor):
    n_row = lax.axis_size("row")
    n_col = lax.axis_size("col")
    count, width = rhs.shape
    leaves, nnear = near_offsets.shape
    pieces = near_blocks.shape[2] // LANES
    near_rows = (
        near_blocks.reshape(leaves, nnear, pieces, LANES).transpose(0, 2, 1, 3).reshape(leaves * pieces * nnear, LANES)
    )
    mixc = mix_col[0]
    mixr = mix_row[0]
    slots = leaves // n_col
    total = n_row * n_col
    operands = (near_offsets.T, rhs, near_rows, v_factor, mixc, mixr, u_factor)
    vmem = pltpu.VMEM
    dma = pltpu.SemaphoreType.DMA
    field = jax.ShapeDtypeStruct((count, width), F32)
    hbm_spec = pl.BlockSpec(memory_space=pltpu.HBM)
    vmem_spec = pl.BlockSpec(memory_space=pltpu.VMEM)
    rhs_v, x, y, coef = pl.pallas_call(
        kernel,
        out_shape=(field, field, field, jax.ShapeDtypeStruct((2, count, LANES), F32)),
        in_specs=[hbm_spec] * 7,
        out_specs=(vmem_spec,) * 4,
        scratch_shapes=[
            pltpu.SMEM((nnear, leaves), jnp.int32),
            vmem(near_rows.shape, BF16),
            vmem(v_factor.shape, BF16),
            vmem(mixc.shape, BF16),
            vmem(mixr.shape, BF16),
            vmem(u_factor.shape, BF16),
            vmem((leaves * LEAF, nnear * LEAF), BF16),
            vmem((leaves * LEAF, LANES), BF16),
            vmem((leaves * RANK, 2 * LANES), BF16),
            vmem((LANES, 256), BF16),
            vmem((256, 256), BF16),
            vmem((256, 256), BF16),
            vmem((2, 2, count, HALO * LEAF), BF16),
            vmem((leaves + 2 * HALO, count, LANES), BF16),
            vmem((count, width), F32),
            vmem((2, QUAD, count, n_col * RANK), BF16),
            vmem((n_col, count, n_row * RANK), BF16),
            vmem((n_col, count, n_row * RANK), BF16),
            vmem((n_col, 2 * LANES, 2 * LANES), BF16),
            vmem((2, n_col, 2 * LANES, LANES), BF16),
            vmem((leaves // QUAD, count, LANES), F32),
            vmem((2, n_col, count, LANES), BF16),
            vmem((2, 2, n_col, count, LANES), BF16),
            vmem((n_row, count, n_col * RANK), BF16),
            vmem((2, n_row, count, n_col * RANK), BF16),
            vmem((2, 2, count, HALO * LEAF), BF16),
            vmem((3, 1, LANES), F32),
            vmem((2, n_col, 1, LANES), F32),
            vmem((total, 1, LANES), F32),
            dma((7,)),
            dma((2, 2)),
            dma((2, 2)),
            dma((2, 2, n_col)),
            dma((2, 2, n_col)),
            dma((2, n_row)),
            dma((2, n_row)),
            dma((2, n_col)),
            dma((2, n_col)),
            dma(()),
            dma(()),
        ],
        compiler_params=pltpu.CompilerParams(
            collective_id=0, has_side_effects=True, vmem_limit_bytes=34 * 1024 * 1024
        ),
        name="gmres",
    )(*(pltpu.with_memory_space_constraint(a, pltpu.HBM) for a in operands))
    return pl.pallas_call(
        finish,
        out_shape=(field, field),
        in_specs=[vmem_spec] * 4,
        out_specs=(hbm_spec,) * 2,
        scratch_shapes=[vmem((count, width), F32), vmem((count, width), F32), dma((len(CHUNKS), 2))],
        compiler_params=pltpu.CompilerParams(vmem_limit_bytes=16 * 1024 * 1024),
        name="combine",
    )(coef, rhs_v, x, y)


def solution(mesh):
    in_specs = (
        P(None, ("row", "col")),
        P(("row", "col"), None, None),
        P(("row", "col"), None),
        P(("row", "col"), None),
        P("row", "col", None, None),
        P("row", "col", None, None),
        P(("row", "col"), None),
    )
    out_specs = (P(None, ("row", "col")), P(None, ("row", "col")))
    return jax.shard_map(body, mesh=mesh, in_specs=in_specs, out_specs=out_specs, check_vma=False)
```
